16 devices in a mesh: cz: 2 (over z), cy: 2 (over y), cx: 4 (over x, core).
Axes of the slice: x: 2, y: 2, z: 2, core: 2. Of those that a mesh axis runs over, the one named last changes fastest.
Arguments:
- x: bfloat16 [768, 3072], P(('cx', 'cz'), 'cy')
- w1: bfloat16 [3072, 12288], P('cy', ('cz', 'cx'))
- w2: bfloat16 [12288, 3072], P('cz', ('cy', 'cx'))
Outputs:
- output: bfloat16 [768, 3072], P(('cx', 'cz'), 'cy')
All inputs are finite; a program needn't handle non-finite values.
Results may differ from the reference program's by a relative error of at most 0.0115084.
Values are sent between devices in bfloat16 or wider.
A program may use at most 1 GiB of HBM per device.

```python
import jax
import jax.numpy as jnp

N = 768
D = 3072
F = 12288


def setup_inputs(seed: int = 0) -> dict:
    k1, k2, k3 = jax.random.split(jax.random.PRNGKey(seed), 3)
    x = jax.random.normal(k1, (N, D), jnp.float32)
    w1 = jax.random.normal(k2, (D, F), jnp.float32) * D ** -0.5
    w2 = jax.random.normal(k3, (F, D), jnp.float32) * F ** -0.5
    return {"x": x.astype(jnp.bfloat16), "w1": w1.astype(jnp.bfloat16), "w2": w2.astype(jnp.bfloat16)}


def reference(x, w1, w2):
    c = jnp.dot(x, w1, preferred_element_type=jnp.float32).astype(jnp.bfloat16)
    h = jax.nn.gelu(c.astype(jnp.float32), approximate=True).astype(jnp.bfloat16)
    return jnp.dot(h, w2, preferred_element_type=jnp.float32).astype(jnp.bfloat16)
```

```python
import functools

import jax
import jax.numpy as jnp
from jax import lax
from jax.experimental import pallas as pl
from jax.experimental.pallas import tpu as pltpu
from jax.sharding import PartitionSpec as P

MESH = pl.DeviceIdType.MESH
R = 48
Q = 96 // R
S = 8 * Q
AHEAD = 1
FWD_X = 1
FWD_DIAG = 2 * Q


def gelu(c):
    return 0.5 * c * (1.0 + jnp.tanh(0.7978845608028654 * (c + 0.044715 * (c * c * c))))


def kernel(x_ref, w1_ref, w2_ref, out_ref, xg, w1v, w2v, ps, pr, hb, zacc, zr, zo, zfin,
           load_sem, x_send, x_sem, xc_sem, p_send, p_sem, h_send, hy_sem, hx_sem, hxd_sem,
           hc_sem, z_send, z_sem, f_send, f_sem):
    cz, cy, cx = lax.axis_index("cz"), lax.axis_index("cy"), lax.axis_index("cx")
    core = lax.rem(cx, 2)
    chip = lax.div(cx, 2)
    cxn = lax.rem(cx + 2, 4)
    cxp = cx + 1 - 2 * core
    y_dev = (cz, 1 - cy, cx)
    z_dev = (1 - cz, cy, cx)
    x_dev = (cz, cy, cxn)
    c_dev = (cz, cy, cxp)
    xc_dev = (cz, cy, lax.rem(cxp + 2, 4))

    def remote(src, dst, send, recv, dev):
        return pltpu.make_async_remote_copy(
            src_ref=src, dst_ref=dst, send_sem=send, recv_sem=recv, device_id=dev, device_id_type=MESH)

    def token(s, xx):
        seg, sub = lax.div(s, Q), lax.rem(s, Q)
        kind = lax.div(seg, 2)
        tx = jnp.where(kind < 2, xx, 1 - xx)
        tz = jnp.where((kind == 0) | (kind == 3), cz, 1 - cz)
        tcx = 2 * tx + lax.rem(seg, 2)
        return tcx, tz, sub

    def index(s, xx):
        tcx, tz, sub = token(s, xx)
        return (tcx * 2 + tz) * Q + sub

    def block(tcx, tz):
        return xg.at[pl.ds((tcx * 2 + tz) * Q, Q)]

    def x_copy(kind, tcx, tz, dev):
        return remote(block(tcx, tz), block(tcx, tz), x_send.at[kind], x_sem.at[kind], dev)

    def xc_copy(kind, tcx, tz):
        return remote(block(tcx, tz), block(tcx, tz), x_send.at[3 + kind], xc_sem.at[kind], c_dev)

    barrier = pltpu.get_barrier_semaphore()
    for dev in (y_dev, z_dev, x_dev, c_dev, xc_dev):
        pl.semaphore_signal(barrier, inc=1, device_id=dev, device_id_type=MESH)
    loads = [
        pltpu.make_async_copy(x_ref, block(cx, cz), load_sem.at[0]),
        pltpu.make_async_copy(w1_ref.at[:, pl.ds(pl.multiple_of((1 - cy) * 768, 128), 768)], w1v.at[0], load_sem.at[1]),
        pltpu.make_async_copy(w1_ref.at[:, pl.ds(pl.multiple_of(cy * 768, 128), 768)], w1v.at[1], load_sem.at[2]),
        pltpu.make_async_copy(w2_ref, w2v, load_sem.at[3]),
    ]
    for load in loads:
        load.start()
    loads[0].wait()
    pl.semaphore_wait(barrier, 5)

    xc_copy(0, cx, cz).start()
    x_copy(0, cx, cz, x_dev).start()
    x_copy(1, cx, cz, z_dev).start()
    loads[1].wait()

    def p_copy(s):
        return remote(ps.at[s], pr.at[s], p_send, p_sem.at[s], y_dev)

    def send_partial(s):
        tcx, tz, sub = token(s, chip)
        kind = lax.div(s, 2 * Q)

        @pl.when((sub == 0) & (lax.rem(tcx, 2) != core))
        def _():
            xc_copy(kind, tcx, tz).wait_recv()

        ps[s] = jnp.dot(xg[(tcx * 2 + tz) * Q + sub], w1v[0], preferred_element_type=jnp.float32)
        p_copy(s).start()

    def h_copy(slot, t, b, recv, dev):
        return remote(hb.at[t, b], hb.at[t, b], h_send.at[slot], recv, dev)

    def own_y(s):
        return h_copy(0, index(s, chip), cx * 2 + cy, hy_sem.at[s], y_dev)

    def own_x(s):
        return h_copy(1, index(s, chip), cx * 2 + cy, hx_sem.at[s], x_dev)

    def own_c(s):
        return h_copy(2, index(s, chip), cx * 2 + cy, hc_sem.at[0, s], c_dev)

    def y_to_x(s):
        return h_copy(3, index(s, chip), cx * 2 + 1 - cy, hxd_sem.at[s], x_dev)

    def y_to_c(s):
        return h_copy(4, index(s, chip), cx * 2 + 1 - cy, hc_sem.at[1, s], c_dev)

    def x_to_c(s):
        return h_copy(5, index(s, 1 - chip), cxn * 2 + cy, hc_sem.at[2, s], c_dev)

    def d_to_c(s):
        return h_copy(6, index(s, 1 - chip), cxn * 2 + 1 - cy, hc_sem.at[3, s], c_dev)

    def make_h(s):
        t = index(s, chip)
        keep = jnp.dot(xg[t], w1v[1], preferred_element_type=jnp.float32)
        p_copy(s).wait_recv()
        c = (keep + pr[s]).astype(jnp.bfloat16).astype(jnp.float32)
        hb[t, cx * 2 + cy] = gelu(c).astype(jnp.bfloat16)
        own_y(s).start()
        own_x(s).start()
        own_c(s).start()

    def layer2(t, xx):
        acc = zacc[t]
        for j in range(4):
            b = xx * 4 + j
            acc += jnp.dot(hb[t, b], w2v[b], preferred_element_type=jnp.float32)
        return acc

    def z_copy(t, tcx, sub):
        return remote(zacc.at[t], zr.at[tcx * Q + sub], z_send, z_sem.at[tcx * Q + sub], z_dev)

    def f_copy(tcx, sub, dev):
        return remote(zo.at[tcx * Q + sub], zfin.at[sub, cx], f_send, f_sem.at[sub, cx], dev)

    def finish(s, xx, local):
        tcx, tz, sub = token(s, xx)
        t = (tcx * 2 + tz) * Q + sub
        kind = lax.div(s, 2 * Q)
        acc = layer2(t, xx)

        @pl.when(kind < 3)
        def _():
            zacc[t] = acc

        @pl.when(kind == 2)
        def _():
            z_copy(t, tcx, sub).start()

        @pl.when(kind == 3)
        def _():
            k = tcx * Q + sub
            remote(zacc.at[t], zr.at[k], z_send, z_sem.at[k], z_dev).wait_recv()
            z = (acc + zr[k]).astype(jnp.bfloat16)
            if local:
                @pl.when(tcx == cx)
                def _():
                    zfin[sub, cx] = z

                @pl.when(tcx != cx)
                def _():
                    zo[k] = z
                    f_copy(tcx, sub, c_dev).start()
            else:
                zo[k] = z
                f_copy(tcx, sub, (cz, cy, tcx)).start()

    for s in range(AHEAD):
        send_partial(s)
    zacc[...] = jnp.zeros_like(zacc)
    loads[2].wait()
    loads[3].wait()

    def body(i, _):
        @pl.when(i + AHEAD < S)
        def _():
            send_partial(i + AHEAD)

        @pl.when(i < S)
        def _():
            make_h(i)

        @pl.when(i == FWD_X)
        def _():
            x_copy(1, cx, 1 - cz, z_dev).wait_recv()
            xc_copy(1, cx, 1 - cz).start()
            x_copy(0, cxn, cz, x_dev).wait_recv()
            x_copy(2, cxn, cz, z_dev).start()
            xc_copy(3, cxn, cz).start()

        @pl.when(i == FWD_DIAG)
        def _():
            x_copy(2, cxn, 1 - cz, z_dev).wait_recv()
            xc_copy(2, cxn, 1 - cz).start()

        @pl.when((i >= 1) & (i < S + 1))
        def _():
            s = i - 1
            own_y(s).wait_recv()
            y_to_x(s).start()
            y_to_c(s).start()
            own_x(s).wait_recv()
            x_to_c(s).start()

        @pl.when((i >= 2) & (i < S + 2))
        def _():
            s = i - 2
            own_c(s).wait_recv()
            y_to_c(s).wait_recv()
            finish(s, chip, False)
            y_to_x(s).wait_recv()
            d_to_c(s).start()

        @pl.when(i >= 3)
        def _():
            s = i - 3
            x_to_c(s).wait_recv()
            d_to_c(s).wait_recv()
            finish(s, 1 - chip, True)

        return 0

    lax.fori_loop(0, S + 3, body, 0)

    for sub in range(Q):
        for j in range(4):
            @pl.when(j != cx)
            def _():
                remote(zo.at[sub], zfin.at[sub, j], f_send, f_sem.at[sub, j], c_dev).wait_recv()
            out_ref[sub, :, j * 384:(j + 1) * 384] = zfin[sub, j]

    for kind, (tcx, tz, dev) in enumerate(((cx, cz, x_dev), (cx, cz, z_dev), (cxn, cz, z_dev))):
        x_copy(kind, tcx, tz, dev).wait_send()
    for kind, (tcx, tz) in enumerate(((cx, cz), (cx, 1 - cz), (cxn, 1 - cz), (cxn, cz))):
        xc_copy(kind, tcx, tz).wait_send()
    pltpu.make_async_copy(ps, pr, p_send).wait()
    for slot in range(7):
        half = hb.at[pl.ds(0, S), 0]
        pltpu.make_async_copy(half, half, h_send.at[slot]).wait()
    half = zacc.at[pl.ds(0, 4 * Q)]
    pltpu.make_async_copy(half, zr, z_send).wait()
    part = zo.at[pl.ds(0, 3 * Q)]
    pltpu.make_async_copy(part, part, f_send).wait()


def solution(mesh):
    def body(x, w1, w2):
        bf16, f32 = jnp.bfloat16, jnp.float32
        dma = pltpu.SemaphoreType.DMA
        out = pl.pallas_call(
            kernel,
            out_shape=jax.ShapeDtypeStruct((Q, R, 1536), bf16),
            in_specs=[pl.BlockSpec(memory_space=pl.ANY)] * 3,
            out_specs=pl.BlockSpec(memory_space=pltpu.VMEM),
            scratch_shapes=[
                pltpu.VMEM((S, R, 1536), bf16),
                pltpu.VMEM((2, 1536, 768), bf16),
                pltpu.VMEM((8, 768, 384), bf16),
                pltpu.VMEM((S, R, 768), f32),
                pltpu.VMEM((S, R, 768), f32),
                pltpu.VMEM((S, 8, R, 768), bf16),
                pltpu.VMEM((S, R, 384), f32),
                pltpu.VMEM((4 * Q, R, 384), f32),
                pltpu.VMEM((4 * Q, R, 384), bf16),
                pltpu.VMEM((Q, 4, R, 384), bf16),
                dma((4,)), dma((7,)), dma((3,)), dma((4,)), dma(()), dma((S,)), dma((7,)), dma((S,)), dma((S,)),
                dma((S,)), dma((4, S)), dma(()), dma((4 * Q,)), dma(()), dma((Q, 4)),
            ],
            compiler_params=pltpu.CompilerParams(
                collective_id=0, has_side_effects=True, vmem_limit_bytes=67_043_328),
        )(x.reshape(Q, R, 1536), w1, w2.reshape(8, 768, 384))
        return out.reshape(96, 1536)

    return jax.shard_map(
        body,
        mesh=mesh,
        in_specs=(P(("cx", "cz"), "cy"), P("cy", ("cz", "cx")), P("cz", ("cy", "cx"))),
        out_specs=P(("cx", "cz"), "cy"),
        check_vma=False,
    )
```

```python
import functools

import jax
import jax.numpy as jnp
from jax import lax
from jax.experimental import pallas as pl
from jax.experimental.pallas import tpu as pltpu
from jax.sharding import PartitionSpec as P

MESH = pl.DeviceIdType.MESH
R = 48
Q = 96 // R
S = 8 * Q
T = S - 2
PIECE = 16
N = R // PIECE
K = 8
FWD_X = 1
FWD_DIAG = 2 * Q


def gelu(c):
    return 0.5 * c * (1.0 + jnp.tanh(0.7978845608028654 * (c + 0.044715 * (c * c * c))))


def kernel(x_ref, w1_ref, w2_ref, out_ref, xg, w1v, w2v, ps, pr, kept, hb, zacc, zr, zo, zfin,
           load_sem, x_send, x_sem, xc_sem, p_send, p_sem, h_send, hy_sem, hx_sem, hd_sem,
           ca_sem, cb_sem, z_send, z_sem, f_send, f_sem):
    cz, cy, cx = lax.axis_index("cz"), lax.axis_index("cy"), lax.axis_index("cx")
    core = lax.rem(cx, 2)
    chip = lax.div(cx, 2)
    cxn = lax.rem(cx + 2, 4)
    cxp = cx + 1 - 2 * core
    y_dev = (cz, 1 - cy, cx)
    z_dev = (1 - cz, cy, cx)
    x_dev = (cz, cy, cxn)
    c_dev = (cz, cy, cxp)
    xc_dev = (cz, cy, lax.rem(cxp + 2, 4))

    def remote(src, dst, send, recv, dev):
        return pltpu.make_async_remote_copy(
            src_ref=src, dst_ref=dst, send_sem=send, recv_sem=recv, device_id=dev, device_id_type=MESH)

    def token(s, xx):
        seg, sub = lax.div(s, Q), lax.rem(s, Q)
        kind = lax.div(seg, 2)
        tx = jnp.where(kind < 2, xx, 1 - xx)
        tz = jnp.where((kind == 0) | (kind == 3), cz, 1 - cz)
        tcx = 2 * tx + lax.rem(seg, 2)
        return tcx, tz, sub

    def index(s, xx):
        tcx, tz, sub = token(s, xx)
        return (tcx * 2 + tz) * Q + sub

    def block(tcx, tz):
        return xg.at[pl.ds((tcx * 2 + tz) * Q, Q)]

    def x_copy(kind, tcx, tz, dev):
        return remote(block(tcx, tz), block(tcx, tz), x_send, x_sem.at[kind], dev)

    def xc_copy(kind, tcx, tz):
        return remote(block(tcx, tz), block(tcx, tz), x_send, xc_sem.at[kind], c_dev)

    def whole(s):
        return s, lax.rem(s, K), pl.ds(0, R)

    def pieces(s):
        return [(s, (T + (s - T) * N + p) % K, pl.ds(p * PIECE, PIECE)) for p in range(N)]

    def p_copy(m):
        s, q, rows = m
        return remote(ps.at[s, rows], pr.at[s, rows], p_send, p_sem.at[q], y_dev)

    def h_copy(t, b, rows, recv, dev):
        return remote(hb.at[t, b, rows], hb.at[t, b, rows], h_send, recv, dev)

    def own_y(m):
        s, q, rows = m
        return h_copy(index(s, chip), cx * 2 + cy, rows, hy_sem.at[q], y_dev)

    def own_x(m):
        s, q, rows = m
        return h_copy(index(s, chip), cx * 2 + cy, rows, hx_sem.at[q], x_dev)

    def y_to_x(m):
        s, q, rows = m
        return h_copy(index(s, chip), cx * 2 + 1 - cy, rows, hd_sem.at[q], x_dev)

    def pair_a(m):
        s, q, rows = m
        return h_copy(index(s, chip), pl.ds(cx * 2, 2), rows, ca_sem.at[q], c_dev)

    def pair_b(m):
        s, q, rows = m
        return h_copy(index(s, 1 - chip), pl.ds(cxn * 2, 2), rows, cb_sem.at[q], c_dev)

    def partial(s):
        tcx, tz, sub = token(s, chip)

        @pl.when((sub == 0) & (lax.rem(tcx, 2) != core))
        def _():
            xc_copy(lax.div(s, 2 * Q), tcx, tz).wait_recv()

        ps[s] = jnp.dot(xg[(tcx * 2 + tz) * Q + sub], w1v[0], preferred_element_type=jnp.float32)

    def keep(s):
        kept[...] = jnp.dot(xg[index(s, chip)], w1v[1], preferred_element_type=jnp.float32)

    def make_h(m):
        s, _, rows = m
        p_copy(m).wait_recv()
        c = (kept[rows] + pr[s, rows]).astype(jnp.bfloat16).astype(jnp.float32)
        hb[index(s, chip), cx * 2 + cy, rows] = gelu(c).astype(jnp.bfloat16)
        own_y(m).start()
        own_x(m).start()

    def layer2(t, xx):
        acc = zacc[t]
        for j in range(4):
            b = xx * 4 + j
            acc += jnp.dot(hb[t, b], w2v[b], preferred_element_type=jnp.float32)
        return acc

    def z_copy(t, k):
        return remote(zacc.at[t], zr.at[k], z_send, z_sem.at[k], z_dev)

    def f_copy(tcx, sub, dev):
        return remote(zo.at[tcx * Q + sub], zfin.at[sub, cx], f_send, f_sem, dev)

    def finish(s, xx, local):
        tcx, tz, sub = token(s, xx)
        t = (tcx * 2 + tz) * Q + sub
        k = tcx * Q + sub
        kind = lax.div(s, 2 * Q)
        acc = layer2(t, xx)

        @pl.when(kind < 3)
        def _():
            zacc[t] = acc

        @pl.when(kind == 2)
        def _():
            z_copy(t, k).start()

        @pl.when(kind == 3)
        def _():
            z_copy(t, k).wait_recv()
            z = (acc + zr[k]).astype(jnp.bfloat16)
            if local:
                @pl.when(tcx == cx)
                def _():
                    zfin[sub, cx] = z

                @pl.when(tcx != cx)
                def _():
                    zo[k] = z
                    f_copy(tcx, sub, c_dev).start()
            else:
                zo[k] = z
                f_copy(tcx, sub, (cz, cy, tcx)).start()

    def relay(m):
        own_y(m).wait_recv()
        y_to_x(m).start()
        pair_a(m).start()
        own_x(m).wait_recv()

    def relay_diag(m):
        y_to_x(m).wait_recv()
        pair_b(m).start()

    def near(s, ms):
        for m in ms:
            pair_a(m).wait_recv()
        finish(s, chip, False)

    def far(s, ms):
        for m in ms:
            pair_b(m).wait_recv()
        finish(s, 1 - chip, True)

    barrier = pltpu.get_barrier_semaphore()
    partners = (y_dev, z_dev, x_dev, c_dev, xc_dev)
    for dev in partners:
        pl.semaphore_signal(barrier, inc=1, device_id=dev, device_id_type=MESH)
    other = pl.multiple_of((1 - cy) * 768, 128)
    mine = pl.multiple_of(cy * 768, 128)
    x_load = pltpu.make_async_copy(x_ref, block(cx, cz), load_sem.at[0])
    first_loads = [
        pltpu.make_async_copy(w1_ref.at[:, pl.ds(other + j * 256, 256)], w1v.at[0, :, pl.ds(j * 256, 256)], load_sem.at[1 + j])
        for j in range(3)]
    keep_load = pltpu.make_async_copy(w1_ref.at[:, pl.ds(mine, 768)], w1v.at[1], load_sem.at[4])
    w2_load = pltpu.make_async_copy(w2_ref, w2v, load_sem.at[5])
    x_load.start()
    for load in first_loads:
        load.start()
    x_load.wait()
    pl.semaphore_wait(barrier, len(partners))
    xc_copy(0, cx, cz).start()
    x_copy(0, cx, cz, x_dev).start()
    x_copy(1, cx, cz, z_dev).start()

    @pl.when(core == 1)
    def _():
        xc_copy(0, cx - 1, cz).wait_recv()

    for j, load in enumerate(first_loads):
        load.wait()
        cols = pl.ds(j * 256, 256)
        ps[0, :, cols] = jnp.dot(xg[index(0, chip)], w1v[0, :, cols], preferred_element_type=jnp.float32)
    p_copy(whole(0)).start()
    keep_load.start()
    w2_load.start()
    zacc[...] = jnp.zeros_like(zacc)

    def body(i, _):
        partial(i + 1)
        p_copy(whole(i + 1)).start()

        @pl.when(i == 0)
        def _():
            keep_load.wait()

        keep(i)
        make_h(whole(i))

        @pl.when(i == FWD_X)
        def _():
            w2_load.wait()
            x_copy(1, cx, 1 - cz, z_dev).wait_recv()
            xc_copy(1, cx, 1 - cz).start()
            x_copy(0, cxn, cz, x_dev).wait_recv()
            x_copy(2, cxn, cz, z_dev).start()
            xc_copy(3, cxn, cz).start()

        @pl.when(i == FWD_DIAG)
        def _():
            x_copy(2, cxn, 1 - cz, z_dev).wait_recv()
            xc_copy(2, cxn, 1 - cz).start()

        @pl.when(i >= 1)
        def _():
            relay(whole(i - 1))

        @pl.when(i >= 2)
        def _():
            m = whole(i - 2)
            near(i - 2, [m])
            relay_diag(m)

        @pl.when(i >= 3)
        def _():
            far(i - 3, [whole(i - 3)])

        return 0

    lax.fori_loop(0, T - 1, body, 0)

    m = pieces(T) + pieces(T + 1)
    w = {s: whole(s) for s in range(T - 4, T)}
    partial(T)
    p_copy(m[0]).start()
    p_copy(m[1]).start()
    keep(T - 1)
    make_h(w[T - 1])
    p_copy(m[2]).start()
    relay(w[T - 2])
    near(T - 3, [w[T - 3]])
    relay_diag(w[T - 3])
    far(T - 4, [w[T - 4]])

    partial(T + 1)
    keep(T)
    make_h(m[0])
    p_copy(m[3]).start()
    relay(w[T - 1])
    near(T - 2, [w[T - 2]])
    relay_diag(w[T - 2])

    make_h(m[1])
    p_copy(m[4]).start()
    far(T - 3, [w[T - 3]])

    make_h(m[2])
    p_copy(m[5]).start()
    relay(m[0])
    keep(T + 1)
    near(T - 1, [w[T - 1]])
    relay_diag(w[T - 1])

    make_h(m[3])
    relay(m[1])
    far(T - 2, [w[T - 2]])

    make_h(m[4])
    relay(m[2])
    far(T - 1, [w[T - 1]])

    make_h(m[5])
    relay(m[3])
    near(T, m[:3])
    relay_diag(m[0])
    relay_diag(m[1])
    relay(m[4])
    relay(m[5])
    relay_diag(m[2])
    far(T, m[:3])
    near(T + 1, m[3:])
    for piece in m[3:]:
        relay_diag(piece)
    far(T + 1, m[3:])

    part = zo.at[pl.ds(0, 3 * Q)]
    pltpu.make_async_copy(part, part, f_sem).wait()
    for sub in range(Q):
        for j in range(4):
            out_ref[sub, :, j * 384:(j + 1) * 384] = zfin[sub, j]

    sent = xg.at[pl.ds(0, 7 * Q)]
    pltpu.make_async_copy(sent, sent, x_send).wait()
    pltpu.make_async_copy(ps, pr, p_send).wait()
    sent = hb.at[:, pl.ds(0, 7)]
    pltpu.make_async_copy(sent, sent, h_send).wait()
    pltpu.make_async_copy(zr, zr, z_send).wait()
    pltpu.make_async_copy(part, part, f_send).wait()


def solution(mesh):
    def body(x, w1, w2):
        bf16, f32 = jnp.bfloat16, jnp.float32
        dma = pltpu.SemaphoreType.DMA
        inputs = (x.reshape(Q, R, 1536), w1, w2.reshape(8, 768, 384))
        out = pl.pallas_call(
            kernel,
            out_shape=jax.ShapeDtypeStruct((Q, R, 1536), bf16),
            in_specs=[pl.BlockSpec(memory_space=pltpu.HBM)] * 3,
            out_specs=pl.BlockSpec(memory_space=pltpu.VMEM),
            scratch_shapes=[
                pltpu.VMEM((S, R, 1536), bf16),
                pltpu.VMEM((2, 1536, 768), bf16),
                pltpu.VMEM((8, 768, 384), bf16),
                pltpu.VMEM((S, R, 768), f32),
                pltpu.VMEM((S, R, 768), f32),
                pltpu.VMEM((R, 768), f32),
                pltpu.VMEM((S, 8, R, 768), bf16),
                pltpu.VMEM((S, R, 384), f32),
                pltpu.VMEM((4 * Q, R, 384), f32),
                pltpu.VMEM((4 * Q, R, 384), bf16),
                pltpu.VMEM((Q, 4, R, 384), bf16),
                dma((6,)), dma(()), dma((3,)), dma((4,)), dma(()), dma((K,)), dma(()), dma((K,)), dma((K,)),
                dma((K,)), dma((K,)), dma((K,)), dma(()), dma((4 * Q,)), dma(()), dma(()),
            ],
            compiler_params=pltpu.CompilerParams(
                collective_id=0, has_side_effects=True, vmem_limit_bytes=40 * 2**20),
        )(*(pltpu.with_memory_space_constraint(v, pltpu.HBM) for v in inputs))
        return out.reshape(96, 1536)

    return jax.shard_map(
        body,
        mesh=mesh,
        in_specs=(P(("cx", "cz"), "cy"), P("cy", ("cz", "cx")), P("cz", ("cy", "cx"))),
        out_specs=P(("cx", "cz"), "cy"),
        check_vma=False,
    )
```

```python
import functools

import jax
import jax.numpy as jnp
from jax import lax
from jax.experimental import pallas as pl
from jax.experimental.pallas import tpu as pltpu
from jax.sharding import PartitionSpec as P

MESH = pl.DeviceIdType.MESH
R = 48
Q = 96 // R
S = 8 * Q
T = S - 2
PIECE = 16
N = R // PIECE
K = 8
KX = 10
FWD_X = 1
FWD_DIAG = 2 * Q


def gelu(c):
    return 0.5 * c * (1.0 + jnp.tanh(0.7978845608028654 * (c + 0.044715 * (c * c * c))))


def kernel(x_ref, w1_ref, w2_ref, out_ref, xg, w1v, w2v, ps, pr, kept, hb, zacc, zr, zo, zfin,
           load_sem, x_send, x_sem, xc_sem, p_send, p_sem, h_send, hy_sem, hx_sem, hd_sem,
           ca_sem, cb_sem, z_send, z_sem, f_send, f_sem):
    cz, cy, cx = lax.axis_index("cz"), lax.axis_index("cy"), lax.axis_index("cx")
    core = lax.rem(cx, 2)
    chip = lax.div(cx, 2)
    cxn = lax.rem(cx + 2, 4)
    cxp = cx + 1 - 2 * core
    y_dev = (cz, 1 - cy, cx)
    z_dev = (1 - cz, cy, cx)
    x_dev = (cz, cy, cxn)
    c_dev = (cz, cy, cxp)
    xc_dev = (cz, cy, lax.rem(cxp + 2, 4))
    d_dev = (cz, 1 - cy, cxn)

    def remote(src, dst, send, recv, dev):
        return pltpu.make_async_remote_copy(
            src_ref=src, dst_ref=dst, send_sem=send, recv_sem=recv, device_id=dev, device_id_type=MESH)

    def token(s, xx, kk):
        seg, sub = lax.div(s, Q), lax.rem(s, Q)
        kind = lax.div(seg, 2)
        tx = jnp.where(kind < 2, xx, 1 - xx)
        tz = jnp.where((kind == 0) | (kind == 3), cz, 1 - cz)
        tcx = 2 * tx + jnp.where(kind == 0, lax.rem(seg + kk, 2), lax.rem(seg, 2))
        return tcx, tz, sub

    def index(s, xx, kk):
        tcx, tz, sub = token(s, xx, kk)
        return (tcx * 2 + tz) * Q + sub

    def block(tcx, tz):
        return xg.at[pl.ds((tcx * 2 + tz) * Q, Q)]

    def x_copy(kind, tcx, tz, dev):
        return remote(block(tcx, tz), block(tcx, tz), x_send, x_sem.at[kind], dev)

    def xc_copy(kind, tcx, tz):
        return remote(block(tcx, tz), block(tcx, tz), x_send, xc_sem.at[kind], c_dev)

    def whole(s):
        return s, s, pl.ds(0, R)

    def pieces(s):
        return [(s, T + (s - T) * N + p, pl.ds(p * PIECE, PIECE)) for p in range(N)]

    def p_copy(m):
        s, q, rows = m
        return remote(ps.at[s, rows], pr.at[s, rows], p_send, p_sem.at[lax.rem(q, K)], y_dev)

    def h_copy(t, b, rows, recv, dev):
        return remote(hb.at[t, b, rows], hb.at[t, b, rows], h_send, recv, dev)

    def own_y(m):
        s, q, rows = m
        return h_copy(index(s, chip, core), cx * 2 + cy, rows, hy_sem.at[lax.rem(q, K)], y_dev)

    def own_x(m):
        s, q, rows = m
        return h_copy(index(s, chip, core), cx * 2 + cy, rows, hx_sem.at[lax.rem(q, KX)], x_dev)

    def y_to_x(m):
        s, q, rows = m
        return h_copy(index(s, chip, core), cx * 2 + 1 - cy, rows, hd_sem.at[lax.rem(q, K)], x_dev)

    def own_d(m, j):
        s, q, rows = m
        return h_copy(index(s, chip, core), cx * 2 + cy, rows, hd_sem.at[K + j], d_dev)

    def pair_a(m):
        s, q, rows = m
        return h_copy(index(s, chip, core), pl.ds(cx * 2, 2), rows, ca_sem.at[lax.rem(q, K)], c_dev)

    def pair_b(m):
        s, q, rows = m
        return h_copy(index(s, 1 - chip, core), pl.ds(cxn * 2, 2), rows, cb_sem.at[lax.rem(q, K)], c_dev)

    def partial(s):
        tcx, tz, sub = token(s, chip, core)

        @pl.when((sub == 0) & (lax.rem(tcx, 2) != core))
        def _():
            xc_copy(lax.div(s, 2 * Q), tcx, tz).wait_recv()

        ps[s] = jnp.dot(xg[(tcx * 2 + tz) * Q + sub], w1v[0], preferred_element_type=jnp.float32)

    def keep(s):
        kept[...] = jnp.dot(xg[index(s, chip, core)], w1v[1], preferred_element_type=jnp.float32)

    def make_h(m):
        s, _, rows = m
        p_copy(m).wait_recv()
        c = (kept[rows] + pr[s, rows]).astype(jnp.bfloat16).astype(jnp.float32)
        hb[index(s, chip, core), cx * 2 + cy, rows] = gelu(c).astype(jnp.bfloat16)
        own_y(m).start()
        own_x(m).start()

    def products(t, xx, kk, rows):
        b = (xx * 2 + kk) * 2
        return (jnp.dot(hb[t, b, rows], w2v[b], preferred_element_type=jnp.float32)
                + jnp.dot(hb[t, b + 1, rows], w2v[b + 1], preferred_element_type=jnp.float32))

    def z_copy(t, k, rows):
        return remote(zacc.at[t, rows], zr.at[k, rows], z_send, z_sem.at[k], z_dev)

    def f_copy(tcx, sub, rows, dev):
        return remote(zo.at[tcx * Q + sub, rows], zfin.at[sub, cx, rows], f_send, f_sem, dev)

    def finish(s, xx, local, rows):
        tcx, tz, sub = token(s, xx, 1)
        t = (tcx * 2 + tz) * Q + sub
        k = tcx * Q + sub
        kind = lax.div(s, 2 * Q)
        if isinstance(s, int) and s >= 2 * Q:
            acc = zacc[t, rows] + products(t, xx, 0, rows) + products(t, xx, 1, rows)
        else:
            t0 = index(s, xx, 0)
            zacc[t0, rows] += products(t0, xx, 0, rows)
            acc = zacc[t, rows] + products(t, xx, 1, rows)

        @pl.when(kind < 3)
        def _():
            zacc[t, rows] = acc

        @pl.when(kind == 2)
        def _():
            z_copy(t, k, rows).start()

        @pl.when(kind == 3)
        def _():
            if rows.start == 0:
                z_copy(t, k, pl.ds(0, R)).wait_recv()
            z = (acc + zr[k, rows]).astype(jnp.bfloat16)
            if local:
                @pl.when(tcx == cx)
                def _():
                    zfin[sub, cx, rows] = z

                @pl.when(tcx != cx)
                def _():
                    zo[k, rows] = z
                    f_copy(tcx, sub, rows, c_dev).start()
            else:
                zo[k, rows] = z
                f_copy(tcx, sub, rows, (cz, cy, tcx)).start()

    def relay(m, ahead=True):
        own_y(m).wait_recv()
        if ahead:
            y_to_x(m).start()
        pair_a(m).start()

    def relay_far(m, j=None):
        own_x(m).wait_recv()
        if j is None:
            y_to_x(m).wait_recv()
        else:
            s, q, rows = m
            h_copy(index(s, 1 - chip, core), cxn * 2 + 1 - cy, rows, hd_sem.at[K + j], d_dev).wait_recv()
        pair_b(m).start()

    def near(s, ms, rows=pl.ds(0, R)):
        for m in ms:
            pair_a(m).wait_recv()
        finish(s, chip, False, rows)

    def far(s, ms, rows=pl.ds(0, R)):
        for m in ms:
            pair_b(m).wait_recv()
        finish(s, 1 - chip, True, rows)

    barrier = pltpu.get_barrier_semaphore()
    partners = (y_dev, z_dev, x_dev, c_dev, xc_dev)
    for dev in partners:
        pl.semaphore_signal(barrier, inc=1, device_id=dev, device_id_type=MESH)
    other = pl.multiple_of((1 - cy) * 768, 128)
    mine = pl.multiple_of(cy * 768, 128)
    x_load = pltpu.make_async_copy(x_ref, block(cx, cz), load_sem.at[0])
    send_load = pltpu.make_async_copy(w1_ref.at[:, pl.ds(other, 768)], w1v.at[0], load_sem.at[1])
    keep_load = pltpu.make_async_copy(w1_ref.at[:, pl.ds(mine, 768)], w1v.at[1], load_sem.at[2])
    w2_load = pltpu.make_async_copy(w2_ref, w2v, load_sem.at[3])
    x_load.start()
    send_load.start()
    x_load.wait()
    send_load.wait()
    keep_load.start()
    w2_load.start()

    partial(0)
    pl.semaphore_wait(barrier, len(partners))
    p_copy(whole(0)).start()
    xc_copy(0, cx, cz).start()
    x_copy(0, cx, cz, x_dev).start()
    x_copy(1, cx, cz, z_dev).start()
    zacc[...] = jnp.zeros_like(zacc)

    def body(i, _):
        partial(i + 1)
        p_copy(whole(i + 1)).start()

        @pl.when(i == 0)
        def _():
            keep_load.wait()

        keep(i)
        make_h(whole(i))

        @pl.when(i == FWD_X)
        def _():
            w2_load.wait()
            x_copy(1, cx, 1 - cz, z_dev).wait_recv()
            xc_copy(1, cx, 1 - cz).start()
            x_copy(0, cxn, cz, x_dev).wait_recv()
            x_copy(2, cxn, cz, z_dev).start()
            xc_copy(3, cxn, cz).start()

        @pl.when(i == FWD_DIAG)
        def _():
            x_copy(2, cxn, 1 - cz, z_dev).wait_recv()
            xc_copy(2, cxn, 1 - cz).start()

        @pl.when(i >= 1)
        def _():
            relay(whole(i - 1))

        @pl.when(i >= 2)
        def _():
            m = whole(i - 2)
            near(i - 2, [m])
            relay_far(m)

        @pl.when(i >= 3)
        def _():
            far(i - 3, [whole(i - 3)])

        return 0

    lax.fori_loop(0, T - 1, body, 0)

    m = pieces(T) + pieces(T + 1)
    w = {s: whole(s) for s in range(T - 4, T)}
    partial(T)
    for piece in m[:3]:
        p_copy(piece).start()
    keep(T - 1)
    make_h(w[T - 1])
    partial(T + 1)
    p_copy(m[3]).start()
    p_copy(m[4]).start()
    relay(w[T - 2])
    near(T - 3, [w[T - 3]])
    relay_far(w[T - 3])
    far(T - 4, [w[T - 4]])
    keep(T)
    make_h(m[0])
    p_copy(m[5]).start()
    near(T - 2, [w[T - 2]])
    make_h(m[1])
    far(T - 3, [w[T - 3]])
    make_h(m[2])
    relay_far(w[T - 2])
    keep(T + 1)
    relay(w[T - 1])
    far(T - 2, [w[T - 2]])
    make_h(m[3])
    near(T - 1, [w[T - 1]])
    make_h(m[4])
    own_d(m[4], 0).start()
    relay(m[0])
    make_h(m[5])
    own_d(m[5], 1).start()
    relay_far(w[T - 1])
    relay(m[1])
    relay(m[2])
    far(T - 1, [w[T - 1]])
    relay(m[3])
    near(T, m[:3])
    relay(m[4], False)
    relay(m[5], False)
    near(T + 1, m[3:5], pl.ds(0, 2 * PIECE))
    relay_far(m[0])
    near(T + 1, m[5:], pl.ds(2 * PIECE, PIECE))
    relay_far(m[1])
    relay_far(m[2])
    relay_far(m[3])
    relay_far(m[4], 0)
    relay_far(m[5], 1)
    far(T, m[:3])
    far(T + 1, m[3:])

    part = zo.at[pl.ds(0, 3 * Q)]
    pltpu.make_async_copy(part, part, f_sem).wait()
    for sub in range(Q):
        for j in range(4):
            out_ref[sub, :, j * 384:(j + 1) * 384] = zfin[sub, j]

    sent = xg.at[pl.ds(0, 7 * Q)]
    pltpu.make_async_copy(sent, sent, x_send).wait()
    pltpu.make_async_copy(ps, pr, p_send).wait()
    sent = hb.at[:, pl.ds(0, 7)]
    pltpu.make_async_copy(sent, sent, h_send).wait()
    pltpu.make_async_copy(zr, zr, z_send).wait()
    pltpu.make_async_copy(part, part, f_send).wait()


def solution(mesh):
    def body(x, w1, w2):
        bf16, f32 = jnp.bfloat16, jnp.float32
        dma = pltpu.SemaphoreType.DMA
        inputs = (x.reshape(Q, R, 1536), w1, w2.reshape(8, 768, 384))
        out = pl.pallas_call(
            kernel,
            out_shape=jax.ShapeDtypeStruct((Q, R, 1536), bf16),
            in_specs=[pl.BlockSpec(memory_space=pltpu.HBM)] * 3,
            out_specs=pl.BlockSpec(memory_space=pltpu.VMEM),
            scratch_shapes=[
                pltpu.VMEM((S, R, 1536), bf16),
                pltpu.VMEM((2, 1536, 768), bf16),
                pltpu.VMEM((8, 768, 384), bf16),
                pltpu.VMEM((S, R, 768), f32),
                pltpu.VMEM((S, R, 768), f32),
                pltpu.VMEM((R, 768), f32),
                pltpu.VMEM((S, 8, R, 768), bf16),
                pltpu.VMEM((S, R, 384), f32),
                pltpu.VMEM((4 * Q, R, 384), f32),
                pltpu.VMEM((4 * Q, R, 384), bf16),
                pltpu.VMEM((Q, 4, R, 384), bf16),
                dma((4,)), dma(()), dma((3,)), dma((4,)), dma(()), dma((K,)), dma(()), dma((K,)), dma((KX,)),
                dma((K + 2,)), dma((K,)), dma((K,)), dma(()), dma((4 * Q,)), dma(()), dma(()),
            ],
            compiler_params=pltpu.CompilerParams(
                collective_id=0, has_side_effects=True, vmem_limit_bytes=40 * 2**20),
        )(*(pltpu.with_memory_space_constraint(v, pltpu.HBM) for v in inputs))
        return out.reshape(96, 1536)

    return jax.shard_map(
        body,
        mesh=mesh,
        in_specs=(P(("cx", "cz"), "cy"), P("cy", ("cz", "cx")), P("cz", ("cy", "cx"))),
        out_specs=P(("cx", "cz"), "cy"),
        check_vma=False,
    )
```

```python
import functools

import jax
import jax.numpy as jnp
from jax import lax
from jax.experimental import pallas as pl
from jax.experimental.pallas import tpu as pltpu
from jax.sharding import PartitionSpec as P

MESH = pl.DeviceIdType.MESH
R = 48
Q = 96 // R
S = 8 * Q
T = S - 2
PIECE = 16
N = R // PIECE
K = 8
KX = 10
FWD_X = 1
FWD_DIAG = 2 * Q


def gelu(c):
    return 0.5 * c * (1.0 + jnp.tanh(0.7978845608028654 * (c + 0.044715 * (c * c * c))))


def kernel(x_ref, w1_ref, w2_ref, out_ref, xg, w1v, w2v, ps, pr, kept, hb, zacc, zr, zo, zfin,
           load_sem, x_send, x_sem, xc_sem, p_send, p_sem, h_send, hy_sem, hx_sem, hd_sem,
           ca_sem, cb_sem, z_send, z_sem, f_send, f_sem):
    cz, cy, cx = lax.axis_index("cz"), lax.axis_index("cy"), lax.axis_index("cx")
    core = lax.rem(cx, 2)
    chip = lax.div(cx, 2)
    cxn = lax.rem(cx + 2, 4)
    cxp = cx + 1 - 2 * core
    y_dev = (cz, 1 - cy, cx)
    z_dev = (1 - cz, cy, cx)
    x_dev = (cz, cy, cxn)
    c_dev = (cz, cy, cxp)
    xc_dev = (cz, cy, lax.rem(cxp + 2, 4))
    d_dev = (cz, 1 - cy, cxn)

    def remote(src, dst, send, recv, dev):
        return pltpu.make_async_remote_copy(
            src_ref=src, dst_ref=dst, send_sem=send, recv_sem=recv, device_id=dev, device_id_type=MESH)

    def apart(f):
        def run(*args):
            @pl.when(cx >= 0)
            def _():
                f(*args)
        return run

    def token(s, xx, kk):
        seg, sub = lax.div(s, Q), lax.rem(s, Q)
        kind = jnp.where(seg < 4, lax.div(seg, 2), 2 + lax.rem(seg, 2))
        tx = jnp.where(kind < 2, xx, 1 - xx)
        tz = jnp.where((kind == 0) | (kind == 3), cz, 1 - cz)
        half = jnp.where(kind == 0, lax.rem(seg + kk, 2), jnp.where(kind == 1, lax.rem(seg, 2), lax.rem(lax.div(seg, 2), 2)))
        return 2 * tx + half, tz, sub, kind

    def index(s, xx, kk):
        tcx, tz, sub, _ = token(s, xx, kk)
        return (tcx * 2 + tz) * Q + sub

    def block(tcx, tz):
        return xg.at[pl.ds((tcx * 2 + tz) * Q, Q)]

    def x_copy(kind, tcx, tz, dev):
        return remote(block(tcx, tz), block(tcx, tz), x_send, x_sem.at[kind], dev)

    def xc_copy(kind, tcx, tz):
        return remote(block(tcx, tz), block(tcx, tz), x_send, xc_sem.at[kind], c_dev)

    def whole(s):
        return s, s, pl.ds(0, R)

    def pieces(s):
        return [(s, T + (s - T) * N + p, pl.ds(p * PIECE, PIECE)) for p in range(N)]

    def p_copy(m):
        s, q, rows = m
        return remote(ps.at[s, rows], pr.at[s, rows], p_send, p_sem.at[lax.rem(q, K)], y_dev)

    def h_copy(t, b, rows, recv, dev):
        return remote(hb.at[t, b, rows], hb.at[t, b, rows], h_send, recv, dev)

    def own_y(m):
        s, q, rows = m
        return h_copy(index(s, chip, core), cx * 2 + cy, rows, hy_sem.at[lax.rem(q, K)], y_dev)

    def own_x(m):
        s, q, rows = m
        return h_copy(index(s, chip, core), cx * 2 + cy, rows, hx_sem.at[lax.rem(q, KX)], x_dev)

    def y_to_x(m):
        s, q, rows = m
        return h_copy(index(s, chip, core), cx * 2 + 1 - cy, rows, hd_sem.at[lax.rem(q, K)], x_dev)

    def own_d(m, j):
        s, q, rows = m
        return h_copy(index(s, chip, core), cx * 2 + cy, rows, hd_sem.at[K + j], d_dev)

    def pair_a(m):
        s, q, rows = m
        return h_copy(index(s, chip, core), pl.ds(cx * 2, 2), rows, ca_sem.at[lax.rem(q, K)], c_dev)

    def pair_b(m):
        s, q, rows = m
        return h_copy(index(s, 1 - chip, core), pl.ds(cxn * 2, 2), rows, cb_sem.at[lax.rem(q, K)], c_dev)

    @apart
    def partial(s):
        tcx, tz, sub, kind = token(s, chip, core)

        @pl.when((sub == 0) & (lax.rem(tcx, 2) != core))
        def _():
            xc_copy(kind, tcx, tz).wait_recv()

        ps[s] = jnp.dot(xg[(tcx * 2 + tz) * Q + sub], w1v[0], preferred_element_type=jnp.float32)

    @apart
    def keep(s):
        kept[...] = jnp.dot(xg[index(s, chip, core)], w1v[1], preferred_element_type=jnp.float32)

    @apart
    def make_h(m):
        s, _, rows = m
        p_copy(m).wait_recv()
        c = (kept[rows] + pr[s, rows]).astype(jnp.bfloat16).astype(jnp.float32)
        hb[index(s, chip, core), cx * 2 + cy, rows] = gelu(c).astype(jnp.bfloat16)
        own_y(m).start()
        own_x(m).start()

    def products(t, xx, kk, rows):
        b = (xx * 2 + kk) * 2
        return (jnp.dot(hb[t, b, rows], w2v[b], preferred_element_type=jnp.float32)
                + jnp.dot(hb[t, b + 1, rows], w2v[b + 1], preferred_element_type=jnp.float32))

    def z_copy(t, k, rows):
        return remote(zacc.at[t, rows], zr.at[k, rows], z_send, z_sem.at[k], z_dev)

    def f_copy(tcx, sub, rows, dev):
        return remote(zo.at[tcx * Q + sub, rows], zfin.at[sub, cx, rows], f_send, f_sem, dev)

    @apart
    def finish(s, xx, local, rows):
        tcx, tz, sub, kind = token(s, xx, 1)
        t = (tcx * 2 + tz) * Q + sub
        k = tcx * Q + sub
        if isinstance(s, int) and s >= 2 * Q:
            acc = zacc[t, rows] + products(t, xx, 0, rows) + products(t, xx, 1, rows)
        else:
            t0 = index(s, xx, 0)
            zacc[t0, rows] += products(t0, xx, 0, rows)
            acc = zacc[t, rows] + products(t, xx, 1, rows)

        @pl.when(kind < 3)
        def _():
            zacc[t, rows] = acc

        @pl.when(kind == 2)
        def _():
            z_copy(t, k, rows).start()

        @pl.when(kind == 3)
        def _():
            if rows.start == 0:
                z_copy(t, k, pl.ds(0, R)).wait_recv()
            z = (acc + zr[k, rows]).astype(jnp.bfloat16)
            if local:
                @pl.when(tcx == cx)
                def _():
                    zfin[sub, cx, rows] = z

                @pl.when(tcx != cx)
                def _():
                    zo[k, rows] = z
                    f_copy(tcx, sub, rows, c_dev).start()
            else:
                zo[k, rows] = z
                f_copy(tcx, sub, rows, (cz, cy, tcx)).start()

    @apart
    def relay(m, ahead=True):
        own_y(m).wait_recv()
        if ahead:
            y_to_x(m).start()
        pair_a(m).start()

    @apart
    def relay_far(m, j=None):
        own_x(m).wait_recv()
        if j is None:
            y_to_x(m).wait_recv()
        else:
            s, q, rows = m
            h_copy(index(s, 1 - chip, core), cxn * 2 + 1 - cy, rows, hd_sem.at[K + j], d_dev).wait_recv()
        pair_b(m).start()

    def near(s, ms, rows=pl.ds(0, R)):
        for m in ms:
            pair_a(m).wait_recv()
        finish(s, chip, False, rows)

    def far(s, ms, rows=pl.ds(0, R)):
        for m in ms:
            pair_b(m).wait_recv()
        finish(s, 1 - chip, True, rows)

    barrier = pltpu.get_barrier_semaphore()
    partners = (y_dev, z_dev, x_dev, c_dev, xc_dev)
    for dev in partners:
        pl.semaphore_signal(barrier, inc=1, device_id=dev, device_id_type=MESH)
    other = pl.multiple_of((1 - cy) * 768, 128)
    mine = pl.multiple_of(cy * 768, 128)
    x_load = pltpu.make_async_copy(x_ref, block(cx, cz), load_sem.at[0])
    send_loads = [
        pltpu.make_async_copy(
            w1_ref.at[:, pl.ds(other + j * 256, 256)], w1v.at[0, :, pl.ds(j * 256, 256)], load_sem.at[1 + j])
        for j in range(3)]
    keep_load = pltpu.make_async_copy(w1_ref.at[:, pl.ds(mine, 768)], w1v.at[1], load_sem.at[4])
    w2_load = pltpu.make_async_copy(w2_ref, w2v, load_sem.at[5])
    x_load.start()
    for load in send_loads:
        load.start()
    x_load.wait()
    for j, load in enumerate(send_loads):
        load.wait()
        cols = pl.ds(j * 256, 256)
        ps[0, :, cols] = jnp.dot(xg[index(0, chip, core)], w1v[0, :, cols], preferred_element_type=jnp.float32)
        if j == 0:
            pl.semaphore_wait(barrier, len(partners))
        remote(ps.at[0, :, cols], pr.at[0, :, cols], p_send, p_sem.at[0], y_dev).start()
    keep_load.start()
    w2_load.start()
    xc_copy(0, cx, cz).start()
    x_copy(0, cx, cz, x_dev).start()
    x_copy(1, cx, cz, z_dev).start()
    zacc[...] = jnp.zeros_like(zacc)

    def body(i, _):
        partial(i + 1)
        p_copy(whole(i + 1)).start()

        @pl.when(i == 0)
        def _():
            keep_load.wait()

        keep(i)
        make_h(whole(i))

        @pl.when(i == FWD_X)
        def _():
            w2_load.wait()
            x_copy(1, cx, 1 - cz, z_dev).wait_recv()
            xc_copy(1, cx, 1 - cz).start()
            x_copy(0, cxn, cz, x_dev).wait_recv()
            x_copy(2, cxn, cz, z_dev).start()
            xc_copy(3, cxn, cz).start()

        @pl.when(i == FWD_DIAG)
        def _():
            x_copy(2, cxn, 1 - cz, z_dev).wait_recv()
            xc_copy(2, cxn, 1 - cz).start()

        @pl.when(i >= 1)
        def _():
            relay(whole(i - 1))

        @pl.when(i >= 2)
        def _():
            m = whole(i - 2)
            near(i - 2, [m])
            relay_far(m)

        @pl.when(i >= 3)
        def _():
            far(i - 3, [whole(i - 3)])

        return 0

    lax.fori_loop(0, T - 1, body, 0)

    m = pieces(T) + pieces(T + 1)
    w = {s: whole(s) for s in range(T - 4, T)}
    partial(T)
    for piece in m[:3]:
        p_copy(piece).start()
    keep(T - 1)
    make_h(w[T - 1])
    partial(T + 1)
    p_copy(m[3]).start()
    p_copy(m[4]).start()
    relay(w[T - 2])
    near(T - 3, [w[T - 3]])
    relay_far(w[T - 3])
    far(T - 4, [w[T - 4]])
    keep(T)
    make_h(m[0])
    p_copy(m[5]).start()
    near(T - 2, [w[T - 2]])
    make_h(m[1])
    far(T - 3, [w[T - 3]])
    make_h(m[2])
    relay_far(w[T - 2])
    keep(T + 1)
    relay(w[T - 1])
    far(T - 2, [w[T - 2]])
    make_h(m[3])
    near(T - 1, [w[T - 1]])
    make_h(m[4])
    own_d(m[4], 0).start()
    relay(m[0])
    make_h(m[5])
    own_d(m[5], 1).start()
    relay_far(w[T - 1])
    relay(m[1])
    relay(m[2])
    far(T - 1, [w[T - 1]])
    relay(m[3])
    near(T, m[:3])
    relay(m[4], False)
    relay(m[5], False)
    near(T + 1, m[3:5], pl.ds(0, 2 * PIECE))
    relay_far(m[0])
    near(T + 1, m[5:], pl.ds(2 * PIECE, PIECE))
    relay_far(m[1])
    relay_far(m[2])
    relay_far(m[3])
    relay_far(m[4], 0)
    relay_far(m[5], 1)
    far(T, m[:3])
    far(T + 1, m[3:])

    part = zo.at[pl.ds(0, 3 * Q)]
    pltpu.make_async_copy(part, part, f_sem).wait()
    for sub in range(Q):
        for j in range(4):
            out_ref[sub, :, j * 384:(j + 1) * 384] = zfin[sub, j]

    sent = xg.at[pl.ds(0, 7 * Q)]
    pltpu.make_async_copy(sent, sent, x_send).wait()
    pltpu.make_async_copy(ps, pr, p_send).wait()
    sent = hb.at[:, pl.ds(0, 7)]
    pltpu.make_async_copy(sent, sent, h_send).wait()
    pltpu.make_async_copy(zr, zr, z_send).wait()
    pltpu.make_async_copy(part, part, f_send).wait()


def solution(mesh):
    def body(x, w1, w2):
        bf16, f32 = jnp.bfloat16, jnp.float32
        dma = pltpu.SemaphoreType.DMA
        inputs = (x.reshape(Q, R, 1536), w1, w2.reshape(8, 768, 384))
        out = pl.pallas_call(
            kernel,
            out_shape=jax.ShapeDtypeStruct((Q, R, 1536), bf16),
            in_specs=[pl.BlockSpec(memory_space=pltpu.HBM)] * 3,
            out_specs=pl.BlockSpec(memory_space=pltpu.VMEM),
            scratch_shapes=[
                pltpu.VMEM((S, R, 1536), bf16),
                pltpu.VMEM((2, 1536, 768), bf16),
                pltpu.VMEM((8, 768, 384), bf16),
                pltpu.VMEM((S, R, 768), f32),
                pltpu.VMEM((S, R, 768), f32),
                pltpu.VMEM((R, 768), f32),
                pltpu.VMEM((S, 8, R, 768), bf16),
                pltpu.VMEM((S, R, 384), f32),
                pltpu.VMEM((4 * Q, R, 384), f32),
                pltpu.VMEM((4 * Q, R, 384), bf16),
                pltpu.VMEM((Q, 4, R, 384), bf16),
                dma((6,)), dma(()), dma((3,)), dma((4,)), dma(()), dma((K,)), dma(()), dma((K,)), dma((KX,)),
                dma((K + 2,)), dma((K,)), dma((K,)), dma(()), dma((4 * Q,)), dma(()), dma(()),
            ],
            compiler_params=pltpu.CompilerParams(
                collective_id=0, has_side_effects=True, vmem_limit_bytes=40 * 2**20),
        )(*(pltpu.with_memory_space_constraint(v, pltpu.HBM) for v in inputs))
        return out.reshape(96, 1536)

    return jax.shard_map(
        body,
        mesh=mesh,
        in_specs=(P(("cx", "cz"), "cy"), P("cy", ("cz", "cx")), P("cz", ("cy", "cx"))),
        out_specs=P(("cx", "cz"), "cy"),
        check_vma=False,
    )
```

```python
import functools

import jax
import jax.numpy as jnp
from jax import lax
from jax.experimental import pallas as pl
from jax.experimental.pallas import tpu as pltpu
from jax.sharding import PartitionSpec as P

MESH = pl.DeviceIdType.MESH
R = 48
Q = 96 // R
S = 8 * Q
T = S - 2
PIECE = 16
N = R // PIECE
K = 8
KX = 10
KB = 4
FWD_X = 1
FWD_DIAG = 2 * Q


def gelu(c):
    return 0.5 * c * (1.0 + jnp.tanh(0.7978845608028654 * (c + 0.044715 * (c * c * c))))


def kernel(x_ref, w1_ref, w2_ref, out_ref, xg, w1v, w2v, ps, pr, kept, hb, zacc, zr, zo, zfin,
           load_sem, x_send, x_sem, xc_sem, p_send, p_sem, h_send, hy_sem, hx_sem, hd_sem,
           ca_sem, cb_sem, z_send, z_sem, f_send, f_sem):
    cz, cy, cx = lax.axis_index("cz"), lax.axis_index("cy"), lax.axis_index("cx")
    core = lax.rem(cx, 2)
    chip = lax.div(cx, 2)
    cxn = lax.rem(cx + 2, 4)
    cxp = cx + 1 - 2 * core
    y_dev = (cz, 1 - cy, cx)
    z_dev = (1 - cz, cy, cx)
    x_dev = (cz, cy, cxn)
    c_dev = (cz, cy, cxp)
    xc_dev = (cz, cy, lax.rem(cxp + 2, 4))
    d_dev = (cz, 1 - cy, cxn)

    def remote(src, dst, send, recv, dev):
        return pltpu.make_async_remote_copy(
            src_ref=src, dst_ref=dst, send_sem=send, recv_sem=recv, device_id=dev, device_id_type=MESH)

    def apart(f):
        def run(*args):
            @pl.when(cx >= 0)
            def _():
                f(*args)
        return run

    def token(s, xx, kk):
        seg, sub = lax.div(s, Q), lax.rem(s, Q)
        kind = jnp.where(seg < 4, lax.div(seg, 2), 2 + lax.rem(seg, 2))
        tx = jnp.where(kind < 2, xx, 1 - xx)
        tz = jnp.where((kind == 0) | (kind == 3), cz, 1 - cz)
        half = jnp.where(kind == 0, lax.rem(seg + kk, 2), jnp.where(kind == 1, lax.rem(seg, 2), lax.rem(lax.div(seg, 2), 2)))
        return 2 * tx + half, tz, sub, kind

    def index(s, xx, kk):
        tcx, tz, sub, _ = token(s, xx, kk)
        return (tcx * 2 + tz) * Q + sub

    def block(tcx, tz):
        return xg.at[pl.ds((tcx * 2 + tz) * Q, Q)]

    def x_copy(kind, tcx, tz, dev):
        return remote(block(tcx, tz), block(tcx, tz), x_send, x_sem.at[kind], dev)

    def xc_copy(kind, tcx, tz):
        return remote(block(tcx, tz), block(tcx, tz), x_send, xc_sem.at[kind], c_dev)

    def whole(s):
        return s, s, pl.ds(0, R)

    def pieces(s):
        return [(s, T + (s - T) * N + p, pl.ds(p * PIECE, PIECE)) for p in range(N)]

    def p_copy(m):
        s, q, rows = m
        return remote(ps.at[s, rows], pr.at[s, rows], p_send, p_sem.at[lax.rem(q, K)], y_dev)

    def h_copy(t, b, rows, recv, dev):
        return remote(hb.at[t, b, rows], hb.at[t, b, rows], h_send, recv, dev)

    def own_y(m):
        s, q, rows = m
        return h_copy(index(s, chip, core), cx * 2 + cy, rows, hy_sem.at[lax.rem(q, K)], y_dev)

    def own_x(m):
        s, q, rows = m
        return h_copy(index(s, chip, core), cx * 2 + cy, rows, hx_sem.at[lax.rem(q, KX)], x_dev)

    def y_to_x(m):
        s, q, rows = m
        return h_copy(index(s, chip, core), cx * 2 + 1 - cy, rows, hd_sem.at[lax.rem(q, K)], x_dev)

    def own_d(m, j):
        s, q, rows = m
        return h_copy(index(s, chip, core), cx * 2 + cy, rows, hd_sem.at[K + j], d_dev)

    def pair_a(m):
        s, q, rows = m
        return h_copy(index(s, chip, core), pl.ds(cx * 2, 2), rows, ca_sem.at[lax.rem(q, K)], c_dev)

    def pair_b(m):
        s, q, rows = m
        return h_copy(index(s, 1 - chip, core), pl.ds(cxn * 2, 2), rows, cb_sem.at[lax.rem(q, KB)], c_dev)

    @apart
    def partial(s):
        tcx, tz, sub, kind = token(s, chip, core)

        @pl.when((sub == 0) & (lax.rem(tcx, 2) != core))
        def _():
            xc_copy(kind, tcx, tz).wait_recv()

        ps[s] = jnp.dot(xg[(tcx * 2 + tz) * Q + sub], w1v[0], preferred_element_type=jnp.float32)

    @apart
    def keep(s):
        kept[...] = jnp.dot(xg[index(s, chip, core)], w1v[1], preferred_element_type=jnp.float32)

    @apart
    def make_h(m):
        s, _, rows = m
        p_copy(m).wait_recv()
        c = (kept[rows] + pr[s, rows]).astype(jnp.bfloat16).astype(jnp.float32)
        hb[index(s, chip, core), cx * 2 + cy, rows] = gelu(c).astype(jnp.bfloat16)
        own_y(m).start()
        own_x(m).start()

    def products(t, xx, kk, rows):
        b = (xx * 2 + kk) * 2
        return (jnp.dot(hb[t, b, rows], w2v[b], preferred_element_type=jnp.float32)
                + jnp.dot(hb[t, b + 1, rows], w2v[b + 1], preferred_element_type=jnp.float32))

    def z_copy(t, k, rows):
        return remote(zacc.at[t, rows], zr.at[k, rows], z_send, z_sem.at[k], z_dev)

    def f_copy(tcx, sub, rows, dev):
        return remote(zo.at[tcx * Q + sub, rows], zfin.at[sub, cx, rows], f_send, f_sem, dev)

    def deliver(acc, t, tcx, sub, k, local, rows):
        if rows.start == 0:
            z_copy(t, k, pl.ds(0, R)).wait_recv()
        z = (acc + zr[k, rows]).astype(jnp.bfloat16)
        if local:
            @pl.when(tcx == cx)
            def _():
                zfin[sub, cx, rows] = z

            @pl.when(tcx != cx)
            def _():
                zo[k, rows] = z
                f_copy(tcx, sub, rows, c_dev).start()
        else:
            zo[k, rows] = z
            f_copy(tcx, sub, rows, (cz, cy, tcx)).start()

    @apart
    def finish(s, xx, local, rows):
        tcx, tz, sub, kind = token(s, xx, 1)
        t = (tcx * 2 + tz) * Q + sub
        k = tcx * Q + sub
        if isinstance(s, int) and s >= 2 * Q:
            acc = zacc[t, rows] + products(t, xx, 0, rows) + products(t, xx, 1, rows)
        else:
            t0 = index(s, xx, 0)
            zacc[t0, rows] += products(t0, xx, 0, rows)
            acc = zacc[t, rows] + products(t, xx, 1, rows)

        @pl.when(kind < 3)
        def _():
            zacc[t, rows] = acc

        @pl.when(kind == 2)
        def _():
            z_copy(t, k, rows).start()

        @pl.when(kind == 3)
        def _():
            deliver(acc, t, tcx, sub, k, local, rows)

    @apart
    def relay(m, ahead=True):
        own_y(m).wait_recv()
        if ahead:
            y_to_x(m).start()
        pair_a(m).start()

    @apart
    def relay_far(m):
        own_x(m).wait_recv()
        y_to_x(m).wait_recv()
        pair_b(m).start()

    def single(m, yy):
        s, _, rows = m
        which = KB + 2 * (s - T) + jnp.where(yy == cy, 0, 1)
        return h_copy(index(s, 1 - chip, core), cxn * 2 + yy, rows, cb_sem.at[which], c_dev)

    @apart
    def relay_x(m):
        own_x(m).wait_recv()
        single(m, cy).start()

    @apart
    def relay_diag(m, j=None):
        if j is None:
            y_to_x(m).wait_recv()
        else:
            s, q, rows = m
            h_copy(index(s, 1 - chip, core), cxn * 2 + 1 - cy, rows, hd_sem.at[K + j], d_dev).wait_recv()
        single(m, 1 - cy).start()

    @apart
    def far_half(yy, final):
        for s in (T, T + 1):
            single((s, s, pl.ds(0, R)), yy).wait_recv()
        tcx, tz, _, _ = token(T, 1 - chip, 1)
        k, first, b = tcx * Q, (tcx * 2 + tz) * Q, (1 - chip) * 4 + yy
        t = pl.ds(first, Q)
        h0, h1 = hb[t, b].reshape(Q * R, 768), hb[t, b + 2].reshape(Q * R, 768)
        acc = zacc[t].reshape(Q * R, 384) + (
            jnp.dot(h0, w2v[b], preferred_element_type=jnp.float32)
            + jnp.dot(h1, w2v[b + 2], preferred_element_type=jnp.float32))
        if not final:
            zacc[t] = acc.reshape(Q, R, 384)
            return
        for sub in range(Q):
            z_copy(first + sub, k + sub, pl.ds(0, R)).wait_recv()
        z = (acc + zr[pl.ds(k, Q)].reshape(Q * R, 384)).astype(jnp.bfloat16).reshape(Q, R, 384)

        @pl.when(tcx == cx)
        def _():
            zfin[:, cx] = z

        @pl.when(tcx != cx)
        def _():
            zo[pl.ds(k, Q)] = z
            remote(zo.at[pl.ds(k, Q)], zfin.at[:, cx], f_send, f_sem, c_dev).start()

    def near(s, ms, rows=pl.ds(0, R)):
        for m in ms:
            pair_a(m).wait_recv()
        finish(s, chip, False, rows)

    def far(s, ms, rows=pl.ds(0, R)):
        for m in ms:
            pair_b(m).wait_recv()
        finish(s, 1 - chip, True, rows)

    barrier = pltpu.get_barrier_semaphore()
    partners = (y_dev, z_dev, x_dev, c_dev, xc_dev)
    for dev in partners:
        pl.semaphore_signal(barrier, inc=1, device_id=dev, device_id_type=MESH)
    other = pl.multiple_of((1 - cy) * 768, 128)
    mine = pl.multiple_of(cy * 768, 128)
    x_load = pltpu.make_async_copy(x_ref, block(cx, cz), load_sem.at[0])
    send_loads = [
        pltpu.make_async_copy(
            w1_ref.at[:, pl.ds(other + j * 256, 256)], w1v.at[0, :, pl.ds(j * 256, 256)], load_sem.at[1 + j])
        for j in range(3)]
    keep_load = pltpu.make_async_copy(w1_ref.at[:, pl.ds(mine, 768)], w1v.at[1], load_sem.at[4])
    w2_load = pltpu.make_async_copy(w2_ref, w2v, load_sem.at[5])
    x_load.start()
    for load in send_loads:
        load.start()
    x_load.wait()
    for j, load in enumerate(send_loads):
        load.wait()
        cols = pl.ds(j * 256, 256)
        ps[0, :, cols] = jnp.dot(xg[index(0, chip, core)], w1v[0, :, cols], preferred_element_type=jnp.float32)
        if j == 0:
            pl.semaphore_wait(barrier, len(partners))
        remote(ps.at[0, :, cols], pr.at[0, :, cols], p_send, p_sem.at[0], y_dev).start()
    keep_load.start()
    w2_load.start()
    xc_copy(0, cx, cz).start()
    x_copy(0, cx, cz, x_dev).start()
    x_copy(1, cx, cz, z_dev).start()
    zacc[...] = jnp.zeros_like(zacc)

    def body(i, _):
        partial(i + 1)
        p_copy(whole(i + 1)).start()

        @pl.when(i == 0)
        def _():
            keep_load.wait()

        keep(i)
        make_h(whole(i))

        @pl.when(i == FWD_X)
        def _():
            w2_load.wait()
            x_copy(1, cx, 1 - cz, z_dev).wait_recv()
            xc_copy(1, cx, 1 - cz).start()
            x_copy(0, cxn, cz, x_dev).wait_recv()
            x_copy(2, cxn, cz, z_dev).start()
            xc_copy(3, cxn, cz).start()

        @pl.when(i == FWD_DIAG)
        def _():
            x_copy(2, cxn, 1 - cz, z_dev).wait_recv()
            xc_copy(2, cxn, 1 - cz).start()

        @pl.when(i >= 1)
        def _():
            relay(whole(i - 1))

        @pl.when(i >= 2)
        def _():
            m = whole(i - 2)
            near(i - 2, [m])
            relay_far(m)

        @pl.when(i >= 3)
        def _():
            far(i - 3, [whole(i - 3)])

        return 0

    lax.fori_loop(0, T - 1, body, 0)

    m = pieces(T) + pieces(T + 1)
    w = {s: whole(s) for s in range(T - 4, T)}
    partial(T)
    for piece in m[:3]:
        p_copy(piece).start()
    keep(T - 1)
    make_h(w[T - 1])
    partial(T + 1)
    p_copy(m[3]).start()
    p_copy(m[4]).start()
    relay(w[T - 2])
    near(T - 3, [w[T - 3]])
    relay_far(w[T - 3])
    far(T - 4, [w[T - 4]])
    keep(T)
    make_h(m[0])
    p_copy(m[5]).start()
    near(T - 2, [w[T - 2]])
    make_h(m[1])
    far(T - 3, [w[T - 3]])
    make_h(m[2])
    relay_far(w[T - 2])
    keep(T + 1)
    relay(w[T - 1])
    far(T - 2, [w[T - 2]])
    make_h(m[3])
    near(T - 1, [w[T - 1]])
    make_h(m[4])
    relay(m[0])
    make_h(m[5])
    own_d(m[4], 0).start()
    own_d(m[5], 1).start()
    relay_far(w[T - 1])

    @pl.when(core == 0)
    def _():
        far(T - 1, [w[T - 1]])

    relay(m[1])
    relay(m[2])

    @pl.when(core == 0)
    def _():
        relay(m[3])
        near(T, m[:3])
        relay(m[4], False)
        relay(m[5], False)
        near(T + 1, m[3:5], pl.ds(0, 2 * PIECE))
        near(T + 1, m[5:], pl.ds(2 * PIECE, PIECE))
        for piece in m:
            relay_x(piece)
        relay_diag(m[0])
        far_half(cy, False)
        relay_diag(m[1])
        relay_diag(m[2])
        relay_diag(m[3])
        relay_diag(m[4], 0)
        relay_diag(m[5], 1)
        far_half(1 - cy, True)


    @pl.when(core == 1)
    def _():
        relay(m[3])
        relay(m[4], False)
        relay(m[5], False)
        far(T - 1, [w[T - 1]])
        near(T, m[:3])
        for piece in m:
            relay_x(piece)
        relay_diag(m[0])
        relay_diag(m[1])
        relay_diag(m[2])
        relay_diag(m[3])
        near(T + 1, m[3:5], pl.ds(0, 2 * PIECE))
        relay_diag(m[4], 0)
        relay_diag(m[5], 1)
        near(T + 1, m[5:], pl.ds(2 * PIECE, PIECE))
        far_half(cy, False)
        far_half(1 - cy, True)

    part = zo.at[pl.ds(0, 3 * Q)]
    pltpu.make_async_copy(part, part, f_sem).wait()
    for sub in range(Q):
        for j in range(4):
            out_ref[sub, :, j * 384:(j + 1) * 384] = zfin[sub, j]

    sent = xg.at[pl.ds(0, 7 * Q)]
    pltpu.make_async_copy(sent, sent, x_send).wait()
    pltpu.make_async_copy(ps, pr, p_send).wait()
    sent = hb.at[:, pl.ds(0, 7)]
    pltpu.make_async_copy(sent, sent, h_send).wait()
    pltpu.make_async_copy(zr, zr, z_send).wait()
    pltpu.make_async_copy(part, part, f_send).wait()


def solution(mesh):
    def body(x, w1, w2):
        bf16, f32 = jnp.bfloat16, jnp.float32
        dma = pltpu.SemaphoreType.DMA
        inputs = (x.reshape(Q, R, 1536), w1, w2.reshape(8, 768, 384))
        out = pl.pallas_call(
            kernel,
            out_shape=jax.ShapeDtypeStruct((Q, R, 1536), bf16),
            in_specs=[pl.BlockSpec(memory_space=pltpu.HBM)] * 3,
            out_specs=pl.BlockSpec(memory_space=pltpu.VMEM),
            scratch_shapes=[
                pltpu.VMEM((S, R, 1536), bf16),
                pltpu.VMEM((2, 1536, 768), bf16),
                pltpu.VMEM((8, 768, 384), bf16),
                pltpu.VMEM((S, R, 768), f32),
                pltpu.VMEM((S, R, 768), f32),
                pltpu.VMEM((R, 768), f32),
                pltpu.VMEM((S, 8, R, 768), bf16),
                pltpu.VMEM((S, R, 384), f32),
                pltpu.VMEM((4 * Q, R, 384), f32),
                pltpu.VMEM((4 * Q, R, 384), bf16),
                pltpu.VMEM((Q, 4, R, 384), bf16),
                dma((6,)), dma(()), dma((3,)), dma((4,)), dma(()), dma((K,)), dma(()), dma((K,)), dma((KX,)),
                dma((K + 2,)), dma((K,)), dma((KB + 4,)), dma(()), dma((4 * Q,)), dma(()), dma(()),
            ],
            compiler_params=pltpu.CompilerParams(
                collective_id=0, has_side_effects=True, vmem_limit_bytes=40 * 2**20),
        )(*(pltpu.with_memory_space_constraint(v, pltpu.HBM) for v in inputs))
        return out.reshape(96, 1536)

    return jax.shard_map(
        body,
        mesh=mesh,
        in_specs=(P(("cx", "cz"), "cy"), P("cy", ("cz", "cx")), P("cz", ("cy", "cx"))),
        out_specs=P(("cx", "cz"), "cy"),
        check_vma=False,
    )
```

```python
import functools

import jax
import jax.numpy as jnp
from jax import lax
from jax.experimental import pallas as pl
from jax.experimental.pallas import tpu as pltpu
from jax.sharding import PartitionSpec as P

MESH = pl.DeviceIdType.MESH
R = 48
Q = 96 // R
S = 8 * Q
T = S - 2
PIECE = 16
N = R // PIECE
K = 8
KX = 10
KB = 4
FWD_X = 1
FWD_DIAG = 2 * Q


def gelu(c):
    return 0.5 * c * (1.0 + jnp.tanh(0.7978845608028654 * (c + 0.044715 * (c * c * c))))


def kernel(x_ref, w1_ref, w2_ref, out_ref, xg, w1v, w2v, ps, pr, kept, hb, zacc, zr, zo, zfin,
           load_sem, x_send, x_sem, xc_sem, p_send, p_sem, h_send, hy_sem, hx_sem, hd_sem,
           ca_sem, cb_sem, z_send, z_sem, f_send, f_sem):
    cz, cy, cx = lax.axis_index("cz"), lax.axis_index("cy"), lax.axis_index("cx")
    core = lax.rem(cx, 2)
    chip = lax.div(cx, 2)
    cxn = lax.rem(cx + 2, 4)
    cxp = cx + 1 - 2 * core
    y_dev = (cz, 1 - cy, cx)
    z_dev = (1 - cz, cy, cx)
    x_dev = (cz, cy, cxn)
    c_dev = (cz, cy, cxp)
    xc_dev = (cz, cy, lax.rem(cxp + 2, 4))
    d_dev = (cz, 1 - cy, cxn)

    def remote(src, dst, send, recv, dev):
        return pltpu.make_async_remote_copy(
            src_ref=src, dst_ref=dst, send_sem=send, recv_sem=recv, device_id=dev, device_id_type=MESH)

    def apart(f):
        def run(*args):
            @pl.when(cx >= 0)
            def _():
                f(*args)
        return run

    def token(s, xx, kk):
        seg, sub = lax.div(s, Q), lax.rem(s, Q)
        kind = jnp.where(seg < 4, lax.div(seg, 2), 2 + lax.rem(seg, 2))
        tx = jnp.where(kind < 2, xx, 1 - xx)
        tz = jnp.where((kind == 0) | (kind == 3), cz, 1 - cz)
        half = jnp.where(kind == 0, lax.rem(seg + kk, 2), jnp.where(kind == 1, lax.rem(seg, 2), lax.rem(lax.div(seg, 2), 2)))
        return 2 * tx + half, tz, sub, kind

    def index(s, xx, kk):
        tcx, tz, sub, _ = token(s, xx, kk)
        return (tcx * 2 + tz) * Q + sub

    def block(tcx, tz):
        return xg.at[pl.ds((tcx * 2 + tz) * Q, Q)]

    def x_copy(kind, tcx, tz, dev):
        return remote(block(tcx, tz), block(tcx, tz), x_send, x_sem.at[kind], dev)

    def xc_copy(kind, tcx, tz):
        return remote(block(tcx, tz), block(tcx, tz), x_send, xc_sem.at[kind], c_dev)

    def whole(s):
        return s, s, pl.ds(0, R)

    def pieces(s):
        return [(s, T + (s - T) * N + p, pl.ds(p * PIECE, PIECE)) for p in range(N)]

    def p_copy(m):
        s, q, rows = m
        return remote(ps.at[s, rows], pr.at[s, rows], p_send, p_sem.at[lax.rem(q, K)], y_dev)

    def h_copy(t, b, rows, recv, dev):
        return remote(hb.at[t, b, rows], hb.at[t, b, rows], h_send, recv, dev)

    def own_y(m):
        s, q, rows = m
        return h_copy(index(s, chip, core), cx * 2 + cy, rows, hy_sem.at[lax.rem(q, K)], y_dev)

    def own_x(m):
        s, q, rows = m
        return h_copy(index(s, chip, core), cx * 2 + cy, rows, hx_sem.at[lax.rem(q, KX)], x_dev)

    def y_to_x(m):
        s, q, rows = m
        return h_copy(index(s, chip, core), cx * 2 + 1 - cy, rows, hd_sem.at[lax.rem(q, K)], x_dev)

    def own_d(m, j):
        s, q, rows = m
        return h_copy(index(s, chip, core), cx * 2 + cy, rows, hd_sem.at[K + j], d_dev)

    def pair_a(m):
        s, q, rows = m
        return h_copy(index(s, chip, core), pl.ds(cx * 2, 2), rows, ca_sem.at[lax.rem(q, K)], c_dev)

    def pair_b(m):
        s, q, rows = m
        return h_copy(index(s, 1 - chip, core), pl.ds(cxn * 2, 2), rows, cb_sem.at[lax.rem(q, KB)], c_dev)

    @apart
    def partial(s):
        tcx, tz, sub, kind = token(s, chip, core)

        @pl.when((sub == 0) & (lax.rem(tcx, 2) != core))
        def _():
            xc_copy(kind, tcx, tz).wait_recv()

        ps[s] = jnp.dot(xg[(tcx * 2 + tz) * Q + sub], w1v[0], preferred_element_type=jnp.float32)

    @apart
    def keep(s):
        kept[...] = jnp.dot(xg[index(s, chip, core)], w1v[1], preferred_element_type=jnp.float32)

    @apart
    def make_h(m):
        s, _, rows = m
        p_copy(m).wait_recv()
        c = (kept[rows] + pr[s, rows]).astype(jnp.bfloat16).astype(jnp.float32)
        hb[index(s, chip, core), cx * 2 + cy, rows] = gelu(c).astype(jnp.bfloat16)
        own_y(m).start()
        own_x(m).start()

    def products(t, xx, kk, rows):
        b = (xx * 2 + kk) * 2
        return (jnp.dot(hb[t, b, rows], w2v[b], preferred_element_type=jnp.float32)
                + jnp.dot(hb[t, b + 1, rows], w2v[b + 1], preferred_element_type=jnp.float32))

    def z_copy(t, k, rows):
        return remote(zacc.at[t, rows], zr.at[k, rows], z_send, z_sem.at[k], z_dev)

    def f_copy(tcx, sub, rows, dev):
        return remote(zo.at[tcx * Q + sub, rows], zfin.at[sub, cx, rows], f_send, f_sem, dev)

    def deliver(acc, t, tcx, sub, k, local, rows):
        if rows.start == 0:
            z_copy(t, k, pl.ds(0, R)).wait_recv()
        z = (acc + zr[k, rows]).astype(jnp.bfloat16)
        if local:
            @pl.when(tcx == cx)
            def _():
                zfin[sub, cx, rows] = z

            @pl.when(tcx != cx)
            def _():
                zo[k, rows] = z
                f_copy(tcx, sub, rows, c_dev).start()
        else:
            zo[k, rows] = z
            f_copy(tcx, sub, rows, (cz, cy, tcx)).start()

    @apart
    def finish(s, xx, local, rows):
        tcx, tz, sub, kind = token(s, xx, 1)
        t = (tcx * 2 + tz) * Q + sub
        k = tcx * Q + sub
        if isinstance(s, int) and s >= 2 * Q:
            acc = zacc[t, rows] + products(t, xx, 0, rows) + products(t, xx, 1, rows)
        else:
            t0 = index(s, xx, 0)
            zacc[t0, rows] += products(t0, xx, 0, rows)
            acc = zacc[t, rows] + products(t, xx, 1, rows)

        @pl.when(kind < 3)
        def _():
            zacc[t, rows] = acc

        @pl.when(kind == 2)
        def _():
            z_copy(t, k, rows).start()

        @pl.when(kind == 3)
        def _():
            deliver(acc, t, tcx, sub, k, local, rows)

    @apart
    def relay(m, ahead=True):
        own_y(m).wait_recv()
        if ahead:
            y_to_x(m).start()
        pair_a(m).start()

    @apart
    def relay_far(m):
        own_x(m).wait_recv()
        y_to_x(m).wait_recv()
        pair_b(m).start()

    def single(m, yy):
        s, _, rows = m
        which = KB + 2 * (s - T) + jnp.where(yy == cy, 0, 1)
        return h_copy(index(s, 1 - chip, core), cxn * 2 + yy, rows, cb_sem.at[which], c_dev)

    @apart
    def relay_x(m):
        own_x(m).wait_recv()
        single(m, cy).start()

    @apart
    def relay_diag(m, j=None):
        if j is None:
            y_to_x(m).wait_recv()
        else:
            s, q, rows = m
            h_copy(index(s, 1 - chip, core), cxn * 2 + 1 - cy, rows, hd_sem.at[K + j], d_dev).wait_recv()
        single(m, 1 - cy).start()

    @apart
    def far_half(yy, final):
        for s in (T, T + 1):
            single((s, s, pl.ds(0, R)), yy).wait_recv()
        tcx, tz, _, _ = token(T, 1 - chip, 1)
        k, first, b = tcx * Q, (tcx * 2 + tz) * Q, (1 - chip) * 4 + yy
        t = pl.ds(first, Q)
        h0, h1 = hb[t, b].reshape(Q * R, 768), hb[t, b + 2].reshape(Q * R, 768)
        acc = zacc[t].reshape(Q * R, 384) + (
            jnp.dot(h0, w2v[b], preferred_element_type=jnp.float32)
            + jnp.dot(h1, w2v[b + 2], preferred_element_type=jnp.float32))
        if not final:
            zacc[t] = acc.reshape(Q, R, 384)
            return
        for sub in range(Q):
            z_copy(first + sub, k + sub, pl.ds(0, R)).wait_recv()
        z = (acc + zr[pl.ds(k, Q)].reshape(Q * R, 384)).astype(jnp.bfloat16).reshape(Q, R, 384)

        @pl.when(tcx == cx)
        def _():
            zfin[:, cx] = z

        @pl.when(tcx != cx)
        def _():
            zo[pl.ds(k, Q)] = z
            remote(zo.at[pl.ds(k, Q)], zfin.at[:, cx], f_send, f_sem, c_dev).start()

    def near(s, ms, rows=pl.ds(0, R)):
        for m in ms:
            pair_a(m).wait_recv()
        finish(s, chip, False, rows)

    def far(s, ms, rows=pl.ds(0, R)):
        for m in ms:
            pair_b(m).wait_recv()
        finish(s, 1 - chip, True, rows)

    barrier = pltpu.get_barrier_semaphore()
    partners = (y_dev, z_dev, x_dev, c_dev, xc_dev)
    for dev in partners:
        pl.semaphore_signal(barrier, inc=1, device_id=dev, device_id_type=MESH)
    other = pl.multiple_of((1 - cy) * 768, 128)
    mine = pl.multiple_of(cy * 768, 128)
    x_load = pltpu.make_async_copy(x_ref, block(cx, cz), load_sem.at[0])
    send_loads = [
        pltpu.make_async_copy(
            w1_ref.at[:, pl.ds(other + j * 256, 256)], w1v.at[0, :, pl.ds(j * 256, 256)], load_sem.at[1 + j])
        for j in range(3)]
    keep_load = pltpu.make_async_copy(w1_ref.at[:, pl.ds(mine, 768)], w1v.at[1], load_sem.at[4])
    w2_load = pltpu.make_async_copy(w2_ref, w2v, load_sem.at[5])
    x_load.start()
    for load in send_loads:
        load.start()
    x_load.wait()
    for j, load in enumerate(send_loads):
        load.wait()
        cols = pl.ds(j * 256, 256)
        ps[0, :, cols] = jnp.dot(xg[index(0, chip, core)], w1v[0, :, cols], preferred_element_type=jnp.float32)
        if j == 0:
            pl.semaphore_wait(barrier, len(partners))
        remote(ps.at[0, :, cols], pr.at[0, :, cols], p_send, p_sem.at[0], y_dev).start()
    keep_load.start()
    w2_load.start()
    xc_copy(0, cx, cz).start()
    x_copy(0, cx, cz, x_dev).start()
    x_copy(1, cx, cz, z_dev).start()
    zacc[...] = jnp.zeros_like(zacc)

    def body(i, _):
        partial(i + 1)
        p_copy(whole(i + 1)).start()

        @pl.when(i == 0)
        def _():
            keep_load.wait()

        keep(i)
        make_h(whole(i))

        @pl.when(i == FWD_X)
        def _():
            w2_load.wait()
            x_copy(1, cx, 1 - cz, z_dev).wait_recv()
            xc_copy(1, cx, 1 - cz).start()
            x_copy(0, cxn, cz, x_dev).wait_recv()
            x_copy(2, cxn, cz, z_dev).start()
            xc_copy(3, cxn, cz).start()

        @pl.when(i == FWD_DIAG)
        def _():
            x_copy(2, cxn, 1 - cz, z_dev).wait_recv()
            xc_copy(2, cxn, 1 - cz).start()

        @pl.when(i >= 1)
        def _():
            relay(whole(i - 1))

        @pl.when(i >= 2)
        def _():
            m = whole(i - 2)
            near(i - 2, [m])
            relay_far(m)

        @pl.when(i >= 3)
        def _():
            far(i - 3, [whole(i - 3)])

        return 0

    lax.fori_loop(0, T - 1, body, 0)

    m = pieces(T) + pieces(T + 1)
    w = {s: whole(s) for s in range(T - 4, T)}
    partial(T)
    for piece in m[:3]:
        p_copy(piece).start()
    keep(T - 1)
    make_h(w[T - 1])
    partial(T + 1)
    p_copy(m[3]).start()
    p_copy(m[4]).start()
    relay(w[T - 2])
    near(T - 3, [w[T - 3]])
    relay_far(w[T - 3])
    far(T - 4, [w[T - 4]])
    keep(T)
    make_h(m[0])
    p_copy(m[5]).start()
    near(T - 2, [w[T - 2]])
    make_h(m[1])
    far(T - 3, [w[T - 3]])
    make_h(m[2])
    relay_far(w[T - 2])
    keep(T + 1)
    relay(w[T - 1])
    far(T - 2, [w[T - 2]])
    make_h(m[3])
    near(T - 1, [w[T - 1]])
    make_h(m[4])
    relay(m[0])
    make_h(m[5])

    @pl.when(core == 0)
    def _():
        own_d(m[4], 0).start()
        own_d(m[5], 1).start()

    relay_far(w[T - 1])

    @pl.when(core == 0)
    def _():
        far(T - 1, [w[T - 1]])

    relay(m[1])
    relay(m[2])

    @pl.when(core == 0)
    def _():
        relay(m[3])
        near(T, m[:3])
        relay(m[4], False)
        relay(m[5], False)
        near(T + 1, m[3:5], pl.ds(0, 2 * PIECE))
        near(T + 1, m[5:], pl.ds(2 * PIECE, PIECE))
        for piece in m:
            relay_x(piece)
        relay_diag(m[0])
        far_half(cy, False)
        relay_diag(m[1])
        relay_diag(m[2])
        relay_diag(m[3])
        relay_diag(m[4], 0)
        relay_diag(m[5], 1)
        far_half(1 - cy, True)


    @pl.when(core == 1)
    def _():
        relay(m[3])
        relay(m[4])
        relay(m[5])
        far(T - 1, [w[T - 1]])
        near(T, m[:3])
        for piece in m:
            relay_x(piece)
        relay_diag(m[0])
        relay_diag(m[1])
        relay_diag(m[2])
        relay_diag(m[3])
        near(T + 1, m[3:5], pl.ds(0, 2 * PIECE))
        relay_diag(m[4])
        relay_diag(m[5])
        near(T + 1, m[5:], pl.ds(2 * PIECE, PIECE))
        far_half(cy, False)
        far_half(1 - cy, True)

    part = zo.at[pl.ds(0, 3 * Q)]
    pltpu.make_async_copy(part, part, f_sem).wait()
    for sub in range(Q):
        for j in range(4):
            out_ref[sub, :, j * 384:(j + 1) * 384] = zfin[sub, j]

    sent = xg.at[pl.ds(0, 7 * Q)]
    pltpu.make_async_copy(sent, sent, x_send).wait()
    pltpu.make_async_copy(ps, pr, p_send).wait()
    sent = hb.at[:, pl.ds(0, 7)]
    pltpu.make_async_copy(sent, sent, h_send).wait()
    pltpu.make_async_copy(zr, zr, z_send).wait()
    pltpu.make_async_copy(part, part, f_send).wait()


def solution(mesh):
    def body(x, w1, w2):
        bf16, f32 = jnp.bfloat16, jnp.float32
        dma = pltpu.SemaphoreType.DMA
        inputs = (x.reshape(Q, R, 1536), w1, w2.reshape(8, 768, 384))
        out = pl.pallas_call(
            kernel,
            out_shape=jax.ShapeDtypeStruct((Q, R, 1536), bf16),
            in_specs=[pl.BlockSpec(memory_space=pltpu.HBM)] * 3,
            out_specs=pl.BlockSpec(memory_space=pltpu.VMEM),
            scratch_shapes=[
                pltpu.VMEM((S, R, 1536), bf16),
                pltpu.VMEM((2, 1536, 768), bf16),
                pltpu.VMEM((8, 768, 384), bf16),
                pltpu.VMEM((S, R, 768), f32),
                pltpu.VMEM((S, R, 768), f32),
                pltpu.VMEM((R, 768), f32),
                pltpu.VMEM((S, 8, R, 768), bf16),
                pltpu.VMEM((S, R, 384), f32),
                pltpu.VMEM((4 * Q, R, 384), f32),
                pltpu.VMEM((4 * Q, R, 384), bf16),
                pltpu.VMEM((Q, 4, R, 384), bf16),
                dma((6,)), dma(()), dma((3,)), dma((4,)), dma(()), dma((K,)), dma(()), dma((K,)), dma((KX,)),
                dma((K + 2,)), dma((K,)), dma((KB + 4,)), dma(()), dma((4 * Q,)), dma(()), dma(()),
            ],
            compiler_params=pltpu.CompilerParams(
                collective_id=0, has_side_effects=True, vmem_limit_bytes=40 * 2**20),
        )(*(pltpu.with_memory_space_constraint(v, pltpu.HBM) for v in inputs))
        return out.reshape(96, 1536)

    return jax.shard_map(
        body,
        mesh=mesh,
        in_specs=(P(("cx", "cz"), "cy"), P("cy", ("cz", "cx")), P("cz", ("cy", "cx"))),
        out_specs=P(("cx", "cz"), "cy"),
        check_vma=False,
    )
```

```python
import functools

import jax
import jax.numpy as jnp
from jax import lax
from jax.experimental import pallas as pl
from jax.experimental.pallas import tpu as pltpu
from jax.sharding import PartitionSpec as P

MESH = pl.DeviceIdType.MESH
R = 48
Q = 96 // R
S = 8 * Q
T = S - 2
PIECE = 16
N = R // PIECE
K = 8
KP = 7
KX = 10
KB = 4
FWD_X = 1
FWD_DIAG = 2 * Q


def gelu(c):
    return 0.5 * c * (1.0 + jnp.tanh(0.7978845608028654 * (c + 0.044715 * (c * c * c))))


def kernel(x_ref, w1_ref, w2_ref, out_ref, xg, w1v, w2v, ps, pr, kept, hb, zacc, zr, zo, zfin,
           load_sem, x_send, x_sem, xc_sem, p_send, p_sem, h_send, hy_sem, hx_sem, hd_sem,
           ca_sem, cb_sem, z_send, z_sem, f_send, f_sem):
    cz, cy, cx = lax.axis_index("cz"), lax.axis_index("cy"), lax.axis_index("cx")
    core = lax.rem(cx, 2)
    chip = lax.div(cx, 2)
    cxn = lax.rem(cx + 2, 4)
    cxp = cx + 1 - 2 * core
    y_dev = (cz, 1 - cy, cx)
    z_dev = (1 - cz, cy, cx)
    x_dev = (cz, cy, cxn)
    c_dev = (cz, cy, cxp)
    xc_dev = (cz, cy, lax.rem(cxp + 2, 4))
    d_dev = (cz, 1 - cy, cxn)

    def remote(src, dst, send, recv, dev):
        return pltpu.make_async_remote_copy(
            src_ref=src, dst_ref=dst, send_sem=send, recv_sem=recv, device_id=dev, device_id_type=MESH)

    def apart(f):
        def run(*args):
            @pl.when(cx >= 0)
            def _():
                f(*args)
        return run

    def token(s, xx, kk):
        seg, sub = lax.div(s, Q), lax.rem(s, Q)
        kind = jnp.where(seg < 4, lax.div(seg, 2), 2 + lax.rem(seg, 2))
        tx = jnp.where(kind < 2, xx, 1 - xx)
        tz = jnp.where((kind == 0) | (kind == 3), cz, 1 - cz)
        half = jnp.where(kind == 0, lax.rem(seg + kk, 2), jnp.where(kind == 1, lax.rem(seg, 2), lax.rem(lax.div(seg, 2), 2)))
        return 2 * tx + half, tz, sub, kind

    def index(s, xx, kk):
        tcx, tz, sub, _ = token(s, xx, kk)
        return (tcx * 2 + tz) * Q + sub

    def block(tcx, tz):
        return xg.at[pl.ds((tcx * 2 + tz) * Q, Q)]

    def x_copy(kind, tcx, tz, dev):
        return remote(block(tcx, tz), block(tcx, tz), x_send, x_sem.at[kind], dev)

    def xc_copy(kind, tcx, tz):
        return remote(block(tcx, tz), block(tcx, tz), x_send, xc_sem.at[kind], c_dev)

    def whole(s):
        return s, s, pl.ds(0, R)

    def pieces(s):
        return [(s, T + (s - T) * N + p, pl.ds(p * PIECE, PIECE)) for p in range(N)]

    def p_copy(m):
        s, q, rows = m
        return remote(ps.at[s, rows], pr.at[s, rows], p_send, p_sem.at[lax.rem(q, KP)], y_dev)

    def h_copy(t, b, rows, recv, dev):
        return remote(hb.at[t, b, rows], hb.at[t, b, rows], h_send, recv, dev)

    def own_y(m):
        s, q, rows = m
        return h_copy(index(s, chip, core), cx * 2 + cy, rows, hy_sem.at[lax.rem(q, KP)], y_dev)

    def own_x(m):
        s, q, rows = m
        return h_copy(index(s, chip, core), cx * 2 + cy, rows, hx_sem.at[lax.rem(q, KX)], x_dev)

    def y_to_x(m):
        s, q, rows = m
        return h_copy(index(s, chip, core), cx * 2 + 1 - cy, rows, hd_sem.at[lax.rem(q, K)], x_dev)

    def own_d(m, j):
        s, q, rows = m
        return h_copy(index(s, chip, core), cx * 2 + cy, rows, hd_sem.at[K + j], d_dev)

    def pair_a(m):
        s, q, rows = m
        return h_copy(index(s, chip, core), pl.ds(cx * 2, 2), rows, ca_sem.at[lax.rem(q, KP)], c_dev)

    def pair_b(m):
        s, q, rows = m
        return h_copy(index(s, 1 - chip, core), pl.ds(cxn * 2, 2), rows, cb_sem.at[lax.rem(q, KB)], c_dev)

    @apart
    def partial(s):
        tcx, tz, sub, kind = token(s, chip, core)

        @pl.when((sub == 0) & (lax.rem(tcx, 2) != core))
        def _():
            xc_copy(kind, tcx, tz).wait_recv()

        ps[s] = jnp.dot(xg[(tcx * 2 + tz) * Q + sub], w1v[0], preferred_element_type=jnp.float32)

    @apart
    def keep(s):
        kept[...] = jnp.dot(xg[index(s, chip, core)], w1v[1], preferred_element_type=jnp.float32)

    @apart
    def make_h(m):
        s, _, rows = m
        p_copy(m).wait_recv()
        c = (kept[rows] + pr[s, rows]).astype(jnp.bfloat16).astype(jnp.float32)
        hb[index(s, chip, core), cx * 2 + cy, rows] = gelu(c).astype(jnp.bfloat16)
        own_y(m).start()
        own_x(m).start()

    def products(t, xx, kk, rows):
        b = (xx * 2 + kk) * 2
        return (jnp.dot(hb[t, b, rows], w2v[b], preferred_element_type=jnp.float32)
                + jnp.dot(hb[t, b + 1, rows], w2v[b + 1], preferred_element_type=jnp.float32))

    def z_copy(t, k, rows):
        return remote(zacc.at[t, rows], zr.at[k, rows], z_send, z_sem.at[k], z_dev)

    def f_copy(tcx, sub, rows, dev):
        return remote(zo.at[tcx * Q + sub, rows], zfin.at[sub, cx, rows], f_send, f_sem, dev)

    def deliver(acc, t, tcx, sub, k, local, rows):
        if rows.start == 0:
            z_copy(t, k, pl.ds(0, R)).wait_recv()
        z = (acc + zr[k, rows]).astype(jnp.bfloat16)
        if local:
            @pl.when(tcx == cx)
            def _():
                zfin[sub, cx, rows] = z

            @pl.when(tcx != cx)
            def _():
                zo[k, rows] = z
                f_copy(tcx, sub, rows, c_dev).start()
        else:
            zo[k, rows] = z
            f_copy(tcx, sub, rows, (cz, cy, tcx)).start()

    @apart
    def finish(s, xx, local, rows):
        tcx, tz, sub, kind = token(s, xx, 1)
        t = (tcx * 2 + tz) * Q + sub
        k = tcx * Q + sub
        if isinstance(s, int) and s >= 2 * Q:
            acc = zacc[t, rows] + products(t, xx, 0, rows) + products(t, xx, 1, rows)
        else:
            t0 = index(s, xx, 0)
            zacc[t0, rows] += products(t0, xx, 0, rows)
            acc = zacc[t, rows] + products(t, xx, 1, rows)

        @pl.when(kind < 3)
        def _():
            zacc[t, rows] = acc

        @pl.when(kind == 2)
        def _():
            z_copy(t, k, rows).start()

        @pl.when(kind == 3)
        def _():
            deliver(acc, t, tcx, sub, k, local, rows)

    @apart
    def relay(m, ahead=True):
        own_y(m).wait_recv()
        if ahead:
            y_to_x(m).start()
        pair_a(m).start()

    @apart
    def relay_far(m):
        own_x(m).wait_recv()
        y_to_x(m).wait_recv()
        pair_b(m).start()

    def single(m, yy):
        s, _, rows = m
        which = KB + 2 * (s - T) + jnp.where(yy == cy, 0, 1)
        return h_copy(index(s, 1 - chip, core), cxn * 2 + yy, rows, cb_sem.at[which], c_dev)

    @apart
    def relay_x(m):
        own_x(m).wait_recv()
        single(m, cy).start()

    @apart
    def relay_diag(m, j=None):
        if j is None:
            y_to_x(m).wait_recv()
        else:
            s, q, rows = m
            h_copy(index(s, 1 - chip, core), cxn * 2 + 1 - cy, rows, hd_sem.at[K + j], d_dev).wait_recv()
        single(m, 1 - cy).start()

    @apart
    def far_half(yy, final):
        for s in (T, T + 1):
            single((s, s, pl.ds(0, R)), yy).wait_recv()
        tcx, tz, _, _ = token(T, 1 - chip, 1)
        k, first, b = tcx * Q, (tcx * 2 + tz) * Q, (1 - chip) * 4 + yy
        t = pl.ds(first, Q)
        h0, h1 = hb[t, b].reshape(Q * R, 768), hb[t, b + 2].reshape(Q * R, 768)
        acc = zacc[t].reshape(Q * R, 384) + (
            jnp.dot(h0, w2v[b], preferred_element_type=jnp.float32)
            + jnp.dot(h1, w2v[b + 2], preferred_element_type=jnp.float32))
        if not final:
            zacc[t] = acc.reshape(Q, R, 384)
            return
        for sub in range(Q):
            z_copy(first + sub, k + sub, pl.ds(0, R)).wait_recv()
        z = (acc + zr[pl.ds(k, Q)].reshape(Q * R, 384)).astype(jnp.bfloat16).reshape(Q, R, 384)

        @pl.when(tcx == cx)
        def _():
            zfin[:, cx] = z

        @pl.when(tcx != cx)
        def _():
            zo[pl.ds(k, Q)] = z
            remote(zo.at[pl.ds(k, Q)], zfin.at[:, cx], f_send, f_sem, c_dev).start()

    def near(s, ms, rows=pl.ds(0, R)):
        for m in ms:
            pair_a(m).wait_recv()
        finish(s, chip, False, rows)

    def far(s, ms, rows=pl.ds(0, R)):
        for m in ms:
            pair_b(m).wait_recv()
        finish(s, 1 - chip, True, rows)

    barrier = pltpu.get_barrier_semaphore()
    partners = (y_dev, z_dev, x_dev, c_dev, xc_dev)
    for dev in partners:
        pl.semaphore_signal(barrier, inc=1, device_id=dev, device_id_type=MESH)
    other = pl.multiple_of((1 - cy) * 768, 128)
    mine = pl.multiple_of(cy * 768, 128)
    x_load = pltpu.make_async_copy(x_ref, block(cx, cz), load_sem.at[0])
    send_loads = [
        pltpu.make_async_copy(
            w1_ref.at[:, pl.ds(other + j * 256, 256)], w1v.at[0, :, pl.ds(j * 256, 256)], load_sem.at[1 + j])
        for j in range(3)]
    keep_load = pltpu.make_async_copy(w1_ref.at[:, pl.ds(mine, 768)], w1v.at[1], load_sem.at[0])
    w2_load = pltpu.make_async_copy(w2_ref, w2v, load_sem.at[1])
    x_load.start()
    for load in send_loads:
        load.start()
    x_load.wait()
    for j, load in enumerate(send_loads):
        load.wait()
        cols = pl.ds(j * 256, 256)
        ps[0, :, cols] = jnp.dot(xg[index(0, chip, core)], w1v[0, :, cols], preferred_element_type=jnp.float32)
        if j == 0:
            pl.semaphore_wait(barrier, len(partners))
        remote(ps.at[0, :, cols], pr.at[0, :, cols], p_send, p_sem.at[0], y_dev).start()
    keep_load.start()
    w2_load.start()
    xc_copy(0, cx, cz).start()
    x_copy(0, cx, cz, x_dev).start()
    x_copy(1, cx, cz, z_dev).start()
    zacc[...] = jnp.zeros_like(zacc)

    def body(i, _):
        partial(i + 1)
        p_copy(whole(i + 1)).start()

        @pl.when(i == 0)
        def _():
            keep_load.wait()

        keep(i)
        make_h(whole(i))

        @pl.when(i == FWD_X)
        def _():
            w2_load.wait()
            x_copy(1, cx, 1 - cz, z_dev).wait_recv()
            xc_copy(1, cx, 1 - cz).start()
            x_copy(0, cxn, cz, x_dev).wait_recv()
            x_copy(2, cxn, cz, z_dev).start()
            xc_copy(3, cxn, cz).start()

        @pl.when(i == FWD_DIAG)
        def _():
            x_copy(2, cxn, 1 - cz, z_dev).wait_recv()
            xc_copy(2, cxn, 1 - cz).start()

        @pl.when(i >= 1)
        def _():
            relay(whole(i - 1))

        @pl.when(i >= 2)
        def _():
            m = whole(i - 2)
            near(i - 2, [m])
            relay_far(m)

        @pl.when(i >= 3)
        def _():
            far(i - 3, [whole(i - 3)])

        return 0

    lax.fori_loop(0, T - 1, body, 0)

    m = pieces(T) + pieces(T + 1)
    w = {s: whole(s) for s in range(T - 4, T)}
    partial(T)
    for piece in m[:3]:
        p_copy(piece).start()
    keep(T - 1)
    make_h(w[T - 1])
    partial(T + 1)
    p_copy(m[3]).start()
    p_copy(m[4]).start()
    relay(w[T - 2])
    near(T - 3, [w[T - 3]])
    relay_far(w[T - 3])
    far(T - 4, [w[T - 4]])
    keep(T)
    make_h(m[0])
    p_copy(m[5]).start()
    near(T - 2, [w[T - 2]])
    make_h(m[1])
    far(T - 3, [w[T - 3]])
    make_h(m[2])
    relay_far(w[T - 2])
    keep(T + 1)
    relay(w[T - 1])
    far(T - 2, [w[T - 2]])
    make_h(m[3])
    near(T - 1, [w[T - 1]])
    make_h(m[4])
    relay(m[0])
    make_h(m[5])

    @pl.when(core == 0)
    def _():
        own_d(m[4], 0).start()
        own_d(m[5], 1).start()

    relay_far(w[T - 1])

    @pl.when(core == 0)
    def _():
        far(T - 1, [w[T - 1]])

    relay(m[1])
    relay(m[2])

    @pl.when(core == 0)
    def _():
        relay(m[3])
        near(T, m[:3])
        relay(m[4], False)
        relay(m[5], False)
        near(T + 1, m[3:5], pl.ds(0, 2 * PIECE))
        near(T + 1, m[5:], pl.ds(2 * PIECE, PIECE))
        for piece in m:
            relay_x(piece)
        relay_diag(m[0])
        far_half(cy, False)
        relay_diag(m[1])
        relay_diag(m[2])
        relay_diag(m[3])
        relay_diag(m[4], 0)
        relay_diag(m[5], 1)
        far_half(1 - cy, True)


    @pl.when(core == 1)
    def _():
        relay(m[3])
        relay(m[4])
        relay(m[5])
        far(T - 1, [w[T - 1]])
        near(T, m[:3])
        for piece in m:
            relay_x(piece)
        relay_diag(m[0])
        relay_diag(m[1])
        relay_diag(m[2])
        relay_diag(m[3])
        near(T + 1, m[3:5], pl.ds(0, 2 * PIECE))
        relay_diag(m[4])
        relay_diag(m[5])
        near(T + 1, m[5:], pl.ds(2 * PIECE, PIECE))
        far_half(cy, False)
        far_half(1 - cy, True)

    part = zo.at[pl.ds(0, 3 * Q)]
    pltpu.make_async_copy(part, part, f_sem).wait()
    for sub in range(Q):
        for j in range(4):
            out_ref[sub, :, j * 384:(j + 1) * 384] = zfin[sub, j]

    sent = xg.at[pl.ds(0, 7 * Q)]
    pltpu.make_async_copy(sent, sent, x_send).wait()
    pltpu.make_async_copy(ps, pr, p_send).wait()
    sent = hb.at[:, pl.ds(0, 7)]
    pltpu.make_async_copy(sent, sent, h_send).wait()
    pltpu.make_async_copy(zr, zr, z_send).wait()
    pltpu.make_async_copy(part, part, f_send).wait()


def solution(mesh):
    def body(x, w1, w2):
        bf16, f32 = jnp.bfloat16, jnp.float32
        dma = pltpu.SemaphoreType.DMA
        inputs = (x.reshape(Q, R, 1536), w1, w2.reshape(8, 768, 384))
        out = pl.pallas_call(
            kernel,
            out_shape=jax.ShapeDtypeStruct((Q, R, 1536), bf16),
            in_specs=[pl.BlockSpec(memory_space=pltpu.HBM)] * 3,
            out_specs=pl.BlockSpec(memory_space=pltpu.VMEM),
            scratch_shapes=[
                pltpu.VMEM((S, R, 1536), bf16),
                pltpu.VMEM((2, 1536, 768), bf16),
                pltpu.VMEM((8, 768, 384), bf16),
                pltpu.VMEM((S, R, 768), f32),
                pltpu.VMEM((S, R, 768), f32),
                pltpu.VMEM((R, 768), f32),
                pltpu.VMEM((S, 8, R, 768), bf16),
                pltpu.VMEM((S, R, 384), f32),
                pltpu.VMEM((4 * Q, R, 384), f32),
                pltpu.VMEM((4 * Q, R, 384), bf16),
                pltpu.VMEM((Q, 4, R, 384), bf16),
                dma((4,)), dma(()), dma((3,)), dma((4,)), dma(()), dma((KP,)), dma(()), dma((KP,)), dma((KX,)),
                dma((K + 2,)), dma((KP,)), dma((KB + 4,)), dma(()), dma((4 * Q,)), dma(()), dma(()),
            ],
            compiler_params=pltpu.CompilerParams(
                collective_id=0, has_side_effects=True, vmem_limit_bytes=40 * 2**20),
        )(*(pltpu.with_memory_space_constraint(v, pltpu.HBM) for v in inputs))
        return out.reshape(96, 1536)

    return jax.shard_map(
        body,
        mesh=mesh,
        in_specs=(P(("cx", "cz"), "cy"), P("cy", ("cz", "cx")), P("cz", ("cy", "cx"))),
        out_specs=P(("cx", "cz"), "cy"),
        check_vma=False,
    )
```

```python
import functools

import jax
import jax.numpy as jnp
from jax import lax
from jax.experimental import pallas as pl
from jax.experimental.pallas import tpu as pltpu
from jax.sharding import PartitionSpec as P

MESH = pl.DeviceIdType.MESH
R = 48
Q = 96 // R
S = 8 * Q
T = S - 2
PIECE = 16
N = R // PIECE
KP = 7
KX = 10
KB = 3
FWD_X = 1
FWD_DIAG = 2 * Q


def gelu(c):
    return 0.5 * c * (1.0 + jnp.tanh(0.7978845608028654 * (c + 0.044715 * (c * c * c))))


def kernel(x_ref, w1_ref, w2_ref, out_ref, xg, w1v, w2v, ps, pr, kept, hb, zacc, zr, zo, zfin,
           load_sem, x_send, x_sem, xc_sem, p_send, p_sem, h_send, hy_sem, hx_sem, hd_sem,
           ca_sem, cb_sem, z_send, z_sem, f_send, f_sem):
    cz, cy, cx = lax.axis_index("cz"), lax.axis_index("cy"), lax.axis_index("cx")
    core = lax.rem(cx, 2)
    chip = lax.div(cx, 2)
    cxn = lax.rem(cx + 2, 4)
    cxp = cx + 1 - 2 * core
    y_dev = (cz, 1 - cy, cx)
    z_dev = (1 - cz, cy, cx)
    x_dev = (cz, cy, cxn)
    c_dev = (cz, cy, cxp)
    xc_dev = (cz, cy, lax.rem(cxp + 2, 4))
    d_dev = (cz, 1 - cy, cxn)

    def remote(src, dst, send, recv, dev):
        return pltpu.make_async_remote_copy(
            src_ref=src, dst_ref=dst, send_sem=send, recv_sem=recv, device_id=dev, device_id_type=MESH)

    def apart(f):
        def run(*args):
            @pl.when(cx >= 0)
            def _():
                f(*args)
        return run

    def token(s, xx, kk):
        seg, sub = lax.div(s, Q), lax.rem(s, Q)
        kind = jnp.where(seg < 4, lax.div(seg, 2), 2 + lax.rem(seg, 2))
        tx = jnp.where(kind < 2, xx, 1 - xx)
        tz = jnp.where((kind == 0) | (kind == 3), cz, 1 - cz)
        half = jnp.where(kind == 0, lax.rem(seg + kk, 2), jnp.where(kind == 1, lax.rem(seg, 2), lax.rem(lax.div(seg, 2), 2)))
        return 2 * tx + half, tz, sub, kind

    def index(s, xx, kk):
        tcx, tz, sub, _ = token(s, xx, kk)
        return (tcx * 2 + tz) * Q + sub

    def block(tcx, tz):
        return xg.at[pl.ds((tcx * 2 + tz) * Q, Q)]

    def x_copy(kind, tcx, tz, dev):
        return remote(block(tcx, tz), block(tcx, tz), x_send, x_sem.at[kind], dev)

    def xc_copy(kind, tcx, tz):
        return remote(block(tcx, tz), block(tcx, tz), x_send, xc_sem.at[kind], c_dev)

    def whole(s):
        return s, s, pl.ds(0, R)

    def pieces(s):
        return [(s, T + (s - T) * N + p, pl.ds(p * PIECE, PIECE)) for p in range(N)]

    def p_copy(m):
        s, q, rows = m
        return remote(ps.at[s, rows], pr.at[s, rows], p_send, p_sem.at[lax.rem(q, KP)], y_dev)

    def h_copy(t, b, rows, recv, dev):
        return remote(hb.at[t, b, rows], hb.at[t, b, rows], h_send, recv, dev)

    def own_y(m):
        s, q, rows = m
        return h_copy(index(s, chip, core), cx * 2 + cy, rows, hy_sem.at[lax.rem(q, KP)], y_dev)

    def own_x(m):
        s, q, rows = m
        return h_copy(index(s, chip, core), cx * 2 + cy, rows, hx_sem.at[lax.rem(q, KX)], x_dev)

    def y_to_x(m):
        s, q, rows = m
        return h_copy(index(s, chip, core), cx * 2 + 1 - cy, rows, hd_sem.at[lax.rem(q, KP)], x_dev)

    def own_d(m, j):
        s, q, rows = m
        return h_copy(index(s, chip, core), cx * 2 + cy, rows, hd_sem.at[KP + j], d_dev)

    def pair_a(m):
        s, q, rows = m
        return h_copy(index(s, chip, core), pl.ds(cx * 2, 2), rows, ca_sem.at[lax.rem(q, KP)], c_dev)

    def pair_b(m):
        s, q, rows = m
        return h_copy(index(s, 1 - chip, core), pl.ds(cxn * 2, 2), rows, cb_sem.at[lax.rem(q, KB)], c_dev)

    @apart
    def partial(s):
        tcx, tz, sub, kind = token(s, chip, core)

        @pl.when((sub == 0) & (lax.rem(tcx, 2) != core))
        def _():
            xc_copy(kind, tcx, tz).wait_recv()

        ps[s] = jnp.dot(xg[(tcx * 2 + tz) * Q + sub], w1v[0], preferred_element_type=jnp.float32)

    @apart
    def keep(s):
        kept[...] = jnp.dot(xg[index(s, chip, core)], w1v[1], preferred_element_type=jnp.float32)

    @apart
    def make_h(m):
        s, _, rows = m
        p_copy(m).wait_recv()
        c = (kept[rows] + pr[s, rows]).astype(jnp.bfloat16).astype(jnp.float32)
        hb[index(s, chip, core), cx * 2 + cy, rows] = gelu(c).astype(jnp.bfloat16)
        own_y(m).start()
        own_x(m).start()

    def products(t, xx, kk, rows):
        b = (xx * 2 + kk) * 2
        return (jnp.dot(hb[t, b, rows], w2v[b], preferred_element_type=jnp.float32)
                + jnp.dot(hb[t, b + 1, rows], w2v[b + 1], preferred_element_type=jnp.float32))

    def z_copy(t, k, rows):
        return remote(zacc.at[t, rows], zr.at[k, rows], z_send, z_sem.at[k], z_dev)

    def f_copy(tcx, sub, rows, dev):
        return remote(zo.at[tcx * Q + sub, rows], zfin.at[sub, cx, rows], f_send, f_sem, dev)

    def deliver(acc, t, tcx, sub, k, local, rows):
        if rows.start == 0:
            z_copy(t, k, pl.ds(0, R)).wait_recv()
        z = (acc + zr[k, rows]).astype(jnp.bfloat16)
        if local:
            @pl.when(tcx == cx)
            def _():
                zfin[sub, cx, rows] = z

            @pl.when(tcx != cx)
            def _():
                zo[k, rows] = z
                f_copy(tcx, sub, rows, c_dev).start()
        else:
            zo[k, rows] = z
            f_copy(tcx, sub, rows, (cz, cy, tcx)).start()

    @apart
    def finish(s, xx, local, rows):
        tcx, tz, sub, kind = token(s, xx, 1)
        t = (tcx * 2 + tz) * Q + sub
        k = tcx * Q + sub
        if isinstance(s, int) and s >= 2 * Q:
            acc = zacc[t, rows] + products(t, xx, 0, rows) + products(t, xx, 1, rows)
        else:
            t0 = index(s, xx, 0)
            zacc[t0, rows] += products(t0, xx, 0, rows)
            acc = zacc[t, rows] + products(t, xx, 1, rows)

        @pl.when(kind < 3)
        def _():
            zacc[t, rows] = acc

        @pl.when(kind == 2)
        def _():
            z_copy(t, k, rows).start()

        @pl.when(kind == 3)
        def _():
            deliver(acc, t, tcx, sub, k, local, rows)

    @apart
    def relay(m, ahead=True):
        own_y(m).wait_recv()
        if ahead:
            y_to_x(m).start()
        pair_a(m).start()

    @apart
    def relay_far(m):
        own_x(m).wait_recv()
        y_to_x(m).wait_recv()
        pair_b(m).start()

    def single(m, yy):
        s, _, rows = m
        which = KB + 2 * (s - T) + jnp.where(yy == cy, 0, 1)
        return h_copy(index(s, 1 - chip, core), cxn * 2 + yy, rows, cb_sem.at[which], c_dev)

    @apart
    def relay_x(m):
        own_x(m).wait_recv()
        single(m, cy).start()

    @apart
    def relay_diag(m, j=None):
        if j is None:
            y_to_x(m).wait_recv()
        else:
            s, q, rows = m
            h_copy(index(s, 1 - chip, core), cxn * 2 + 1 - cy, rows, hd_sem.at[KP + j], d_dev).wait_recv()
        single(m, 1 - cy).start()

    @apart
    def far_half(yy, final):
        for s in (T, T + 1):
            single((s, s, pl.ds(0, R)), yy).wait_recv()
        tcx, tz, _, _ = token(T, 1 - chip, 1)
        k, first, b = tcx * Q, (tcx * 2 + tz) * Q, (1 - chip) * 4 + yy
        t = pl.ds(first, Q)
        h0, h1 = hb[t, b].reshape(Q * R, 768), hb[t, b + 2].reshape(Q * R, 768)
        acc = zacc[t].reshape(Q * R, 384) + (
            jnp.dot(h0, w2v[b], preferred_element_type=jnp.float32)
            + jnp.dot(h1, w2v[b + 2], preferred_element_type=jnp.float32))
        if not final:
            zacc[t] = acc.reshape(Q, R, 384)
            return
        for sub in range(Q):
            z_copy(first + sub, k + sub, pl.ds(0, R)).wait_recv()
        z = (acc + zr[pl.ds(k, Q)].reshape(Q * R, 384)).astype(jnp.bfloat16).reshape(Q, R, 384)

        @pl.when(tcx == cx)
        def _():
            zfin[:, cx] = z

        @pl.when(tcx != cx)
        def _():
            zo[pl.ds(k, Q)] = z
            remote(zo.at[pl.ds(k, Q)], zfin.at[:, cx], f_send, f_sem, c_dev).start()

    def near(s, ms, rows=pl.ds(0, R)):
        for m in ms:
            pair_a(m).wait_recv()
        finish(s, chip, False, rows)

    def far(s, ms, rows=pl.ds(0, R)):
        for m in ms:
            pair_b(m).wait_recv()
        finish(s, 1 - chip, True, rows)

    barrier = pltpu.get_barrier_semaphore()
    partners = (y_dev, z_dev, x_dev, c_dev, xc_dev)
    for dev in partners:
        pl.semaphore_signal(barrier, inc=1, device_id=dev, device_id_type=MESH)
    other = pl.multiple_of((1 - cy) * 768, 128)
    mine = pl.multiple_of(cy * 768, 128)
    x_load = pltpu.make_async_copy(x_ref, block(cx, cz), load_sem.at[0])
    send_loads = [
        pltpu.make_async_copy(
            w1_ref.at[:, pl.ds(other + j * 256, 256)], w1v.at[0, :, pl.ds(j * 256, 256)], load_sem.at[1 + j])
        for j in range(3)]
    keep_load = pltpu.make_async_copy(w1_ref.at[:, pl.ds(mine, 768)], w1v.at[1], load_sem.at[0])
    w2_load = pltpu.make_async_copy(w2_ref, w2v, load_sem.at[1])
    x_load.start()
    for load in send_loads:
        load.start()
    x_load.wait()
    for j, load in enumerate(send_loads):
        load.wait()
        cols = pl.ds(j * 256, 256)
        ps[0, :, cols] = jnp.dot(xg[index(0, chip, core)], w1v[0, :, cols], preferred_element_type=jnp.float32)
        if j == 0:
            pl.semaphore_wait(barrier, len(partners))
        remote(ps.at[0, :, cols], pr.at[0, :, cols], p_send, p_sem.at[0], y_dev).start()
    keep_load.start()
    w2_load.start()
    xc_copy(0, cx, cz).start()
    x_copy(0, cx, cz, x_dev).start()
    x_copy(1, cx, cz, z_dev).start()
    zacc[...] = jnp.zeros_like(zacc)

    def body(i, _):
        partial(i + 1)
        p_copy(whole(i + 1)).start()

        @pl.when(i == 0)
        def _():
            keep_load.wait()

        keep(i)
        make_h(whole(i))

        @pl.when(i == FWD_X)
        def _():
            w2_load.wait()
            x_copy(1, cx, 1 - cz, z_dev).wait_recv()
            xc_copy(1, cx, 1 - cz).start()
            x_copy(0, cxn, cz, x_dev).wait_recv()
            x_copy(2, cxn, cz, z_dev).start()
            xc_copy(3, cxn, cz).start()

        @pl.when(i == FWD_DIAG)
        def _():
            x_copy(2, cxn, 1 - cz, z_dev).wait_recv()
            xc_copy(2, cxn, 1 - cz).start()

        @pl.when(i >= 1)
        def _():
            relay(whole(i - 1))

        @pl.when(i >= 2)
        def _():
            m = whole(i - 2)
            near(i - 2, [m])
            relay_far(m)

        @pl.when(i >= 3)
        def _():
            far(i - 3, [whole(i - 3)])

        return 0

    lax.fori_loop(0, T - 1, body, 0)

    m = pieces(T) + pieces(T + 1)
    w = {s: whole(s) for s in range(T - 4, T)}
    partial(T)
    for piece in m[:3]:
        p_copy(piece).start()
    keep(T - 1)
    make_h(w[T - 1])
    partial(T + 1)
    p_copy(m[3]).start()
    p_copy(m[4]).start()
    relay(w[T - 2])
    near(T - 3, [w[T - 3]])
    relay_far(w[T - 3])
    far(T - 4, [w[T - 4]])
    keep(T)
    make_h(m[0])
    p_copy(m[5]).start()
    near(T - 2, [w[T - 2]])
    make_h(m[1])
    far(T - 3, [w[T - 3]])
    make_h(m[2])
    relay_far(w[T - 2])
    keep(T + 1)
    relay(w[T - 1])
    far(T - 2, [w[T - 2]])
    make_h(m[3])
    near(T - 1, [w[T - 1]])
    make_h(m[4])
    relay(m[0])
    make_h(m[5])

    @pl.when(core == 0)
    def _():
        own_d(m[4], 0).start()
        own_d(m[5], 1).start()

    relay_far(w[T - 1])

    @pl.when(core == 0)
    def _():
        far(T - 1, [w[T - 1]])

    relay(m[1])
    relay(m[2])

    @pl.when(core == 0)
    def _():
        relay(m[3])
        near(T, m[:3])
        relay(m[4], False)
        relay(m[5], False)
        near(T + 1, m[3:5], pl.ds(0, 2 * PIECE))
        near(T + 1, m[5:], pl.ds(2 * PIECE, PIECE))
        for piece in m:
            relay_x(piece)
        relay_diag(m[0])
        far_half(cy, False)
        relay_diag(m[1])
        relay_diag(m[2])
        relay_diag(m[3])
        relay_diag(m[4], 0)
        relay_diag(m[5], 1)
        far_half(1 - cy, True)


    @pl.when(core == 1)
    def _():
        relay(m[3])
        relay(m[4])
        relay(m[5])
        far(T - 1, [w[T - 1]])
        near(T, m[:3])
        for piece in m:
            relay_x(piece)
        relay_diag(m[0])
        relay_diag(m[1])
        relay_diag(m[2])
        relay_diag(m[3])
        near(T + 1, m[3:5], pl.ds(0, 2 * PIECE))
        relay_diag(m[4])
        relay_diag(m[5])
        near(T + 1, m[5:], pl.ds(2 * PIECE, PIECE))
        far_half(cy, False)
        far_half(1 - cy, True)

    part = zo.at[pl.ds(0, 3 * Q)]
    pltpu.make_async_copy(part, part, f_sem).wait()
    for sub in range(Q):
        for j in range(4):
            out_ref[sub, :, j * 384:(j + 1) * 384] = zfin[sub, j]

    sent = xg.at[pl.ds(0, 7 * Q)]
    pltpu.make_async_copy(sent, sent, x_send).wait()
    pltpu.make_async_copy(ps, pr, p_send).wait()
    sent = hb.at[:, pl.ds(0, 7)]
    pltpu.make_async_copy(sent, sent, h_send).wait()
    pltpu.make_async_copy(zr, zr, z_send).wait()
    pltpu.make_async_copy(part, part, f_send).wait()


def solution(mesh):
    def body(x, w1, w2):
        bf16, f32 = jnp.bfloat16, jnp.float32
        dma = pltpu.SemaphoreType.DMA
        inputs = (x.reshape(Q, R, 1536), w1, w2.reshape(8, 768, 384))
        out = pl.pallas_call(
            kernel,
            out_shape=jax.ShapeDtypeStruct((Q, R, 1536), bf16),
            in_specs=[pl.BlockSpec(memory_space=pltpu.HBM)] * 3,
            out_specs=pl.BlockSpec(memory_space=pltpu.VMEM),
            scratch_shapes=[
                pltpu.VMEM((S, R, 1536), bf16),
                pltpu.VMEM((2, 1536, 768), bf16),
                pltpu.VMEM((8, 768, 384), bf16),
                pltpu.VMEM((S, R, 768), f32),
                pltpu.VMEM((S, R, 768), f32),
                pltpu.VMEM((R, 768), f32),
                pltpu.VMEM((S, 8, R, 768), bf16),
                pltpu.VMEM((S, R, 384), f32),
                pltpu.VMEM((4 * Q, R, 384), f32),
                pltpu.VMEM((4 * Q, R, 384), bf16),
                pltpu.VMEM((Q, 4, R, 384), bf16),
                dma((4,)), dma(()), dma((3,)), dma((4,)), dma(()), dma((KP,)), dma(()), dma((KP,)), dma((KX,)),
                dma((KP + 2,)), dma((KP,)), dma((KB + 4,)), dma(()), dma((4 * Q,)), dma(()), dma(()),
            ],
            compiler_params=pltpu.CompilerParams(
                collective_id=0, has_side_effects=True, vmem_limit_bytes=40 * 2**20),
        )(*(pltpu.with_memory_space_constraint(v, pltpu.HBM) for v in inputs))
        return out.reshape(96, 1536)

    return jax.shard_map(
        body,
        mesh=mesh,
        in_specs=(P(("cx", "cz"), "cy"), P("cy", ("cz", "cx")), P("cz", ("cy", "cx"))),
        out_specs=P(("cx", "cz"), "cy"),
        check_vma=False,
    )
```
